128 devices in a mesh: tm: 8 (over x, core), space: 16 (over z, y).
Axes of the slice: x: 4, y: 4, z: 4, core: 2. Of those that a mesh axis runs over, the one named last changes fastest.
Arguments:
- speed: float32 [32, 16, 128], P('space'), may hold values from 0.5 to 1.5
- forcing: float32 [32, 32, 16, 128], P('tm', 'space'), may hold values from -1.8 to 1.8
- guess: float32 [8, 4, 32, 16, 128], P('tm', None, 'space'), may hold values from -8 to 8
- basis: float32 [8, 64, 4, 32, 16, 128], P('tm', None, None, 'space'), may hold values from -1 to 1, as said below
Outputs:
- states: float32 [32, 4, 32, 16, 128], P('tm', None, 'space')
- coords: float32 [8, 64], P('tm')
The draws below stay inside these ranges and needn't reach their ends.
Inputs may be any that keep to these rules, and one draw needn't show every extreme that they name: The columns of each basis[k] are linearly independent.
All inputs are finite; a program needn't handle non-finite values.
Results may differ from the reference program's by a relative error of at most 0.00018.
Values sent between devices are 32-bit elements; how exact they have to be, the bound alone decides.
No kernel may reach another device: no remote copies, remote signals or barrier semaphores. Data moves between devices by JAX's collectives and lax.ppermute only.
A program may use at most 128 MiB of HBM per device.

```python
import jax
import jax.numpy as jnp
from jax import lax

NX = 16
NY = 128
RANK = 64
NZ = 32
NT = 32
N_TM = 8


DT = 0.045


def shifted_ahead_drawn(values, axis):
    size = values.shape[axis]
    rest = lax.slice_in_dim(values, 1, size, axis=axis)
    border = jnp.zeros_like(lax.slice_in_dim(values, 0, 1, axis=axis))
    return jnp.concatenate([rest, border], axis=axis)


def shifted_behind_drawn(values, axis):
    size = values.shape[axis]
    rest = lax.slice_in_dim(values, 0, size - 1, axis=axis)
    border = jnp.zeros_like(lax.slice_in_dim(values, 0, 1, axis=axis))
    return jnp.concatenate([border, rest], axis=axis)


def fine_advance(state, speed_sq):
    pressure = state[..., 0, :, :, :]
    depth = pressure.ndim
    flow_x = state[..., 1, :, :, :] - DT * (shifted_ahead_drawn(pressure, depth - 2) - pressure)
    flow_y = state[..., 2, :, :, :] - DT * (shifted_ahead_drawn(pressure, depth - 1) - pressure)
    flow_z = state[..., 3, :, :, :] - DT * (shifted_ahead_drawn(pressure, depth - 3) - pressure)
    diverge = flow_x - shifted_behind_drawn(flow_x, depth - 2) + (flow_y - shifted_behind_drawn(flow_y, depth - 1)) + (flow_z - shifted_behind_drawn(flow_z, depth - 3))
    fresh = pressure - DT * speed_sq * diverge
    return jnp.stack([fresh, flow_x, flow_y, flow_z], axis=depth - 3)


def speed_field(key):
    log_speed = jax.random.uniform(jax.random.fold_in(key, 202), (NZ, NX, NY), jnp.float32, jnp.log(0.5), jnp.log(1.5))
    return jnp.clip(jnp.exp(log_speed), 0.5, 1.5)


def pattern_block(key, block_index):
    return jax.random.normal(jax.random.fold_in(jax.random.fold_in(key, 101), block_index), (RANK, 4, NZ, NX, NY), jnp.float32)


def draw_speed(key, part):
    return speed_field(key)


def draw_guess(key, part):
    mixing = jax.random.normal(jax.random.fold_in(key, 404), (N_TM, RANK), jnp.float32)

    def aligned(block_index):
        block = pattern_block(key, block_index)
        factors = mixing[block_index][:, None, None, None, None]
        return jnp.sum(factors * block, axis=0) / jnp.sqrt(jnp.float32(RANK))
    aligned_all = lax.map(aligned, jnp.arange(N_TM, dtype=jnp.int32))
    rough_part = jax.random.normal(jax.random.fold_in(key, 303), aligned_all.shape, jnp.float32)
    strength = 1.0
    return jnp.clip(rough_part + strength * aligned_all, -8.0, 8.0)


def draw_basis(key, part):
    speed_sq = jnp.square(speed_field(key))
    cell_count = 4 * NZ * NX * NY
    blend_weight = 0.0
    least_scale = 0.3
    most_scale = 3.0
    scales = jnp.exp(jax.random.uniform(jax.random.fold_in(key, 505), (N_TM, RANK), jnp.float32, jnp.log(least_scale), jnp.log(most_scale)))

    def column_block(block_index):
        source = (block_index + N_TM - 2) % N_TM
        moved_block = pattern_block(key, source)
        for repeat in range(4):
            moved_block = fine_advance(moved_block, speed_sq)
        common = jnp.sum(moved_block, axis=0) / jnp.sqrt(jnp.float32(RANK))
        mixed_columns = moved_block + blend_weight * common[None]
        column_scale = scales[block_index] / jnp.sqrt(jnp.float32(cell_count))
        return mixed_columns * column_scale[:, None, None, None, None]
    columns = lax.map(column_block, jnp.arange(N_TM, dtype=jnp.int32))
    return jnp.clip(columns, -1.0, 1.0)


def steps_of(own_key, extent, cuts, least, largest):
    level = 1.0
    for axis_at, shards_of in cuts:
        draws = jax.random.uniform(jax.random.fold_in(jax.random.fold_in(own_key, 6), axis_at), (shards_of,), jnp.float32, least / len(cuts), largest / len(cuts))
        level = level * jnp.repeat(jnp.exp(draws), extent[axis_at] // shards_of).reshape((-1,) + (1,) * (len(extent) - 1 - axis_at))
    return level


def bell_draw(own_key, shape, scale, most, cuts=(), held_as=jnp.bfloat16):
    drawn = scale * jax.random.normal(own_key, shape, jnp.float32)
    if cuts:
        drawn = drawn * steps_of(own_key, shape, cuts, -0.22, 0.18)
    return jnp.clip(drawn, -most, most).astype(held_as)


def setup_inputs(seed: int = 0) -> dict:
    key_list = jax.random.split(jax.random.key(seed), 5)
    return {
        "speed": draw_speed(jax.random.fold_in(key_list[4], 71), 0),
        "forcing": bell_draw(key_list[1], (NT, NZ, NX, NY), 0.3, 1.8, ((0, 8), (1, 16)), jnp.float32),
        "guess": draw_guess(jax.random.fold_in(key_list[4], 71), 0),
        "basis": draw_basis(jax.random.fold_in(key_list[4], 71), 0),
    }


DT = 0.045
exact_mode = lax.Precision.HIGHEST

def shifted_ahead(values, axis):
    size = values.shape[axis]
    rest = lax.slice_in_dim(values, 1, size, axis=axis)
    border = jnp.zeros_like(lax.slice_in_dim(values, 0, 1, axis=axis))
    return jnp.concatenate([rest, border], axis=axis)

def shifted_behind(values, axis):
    size = values.shape[axis]
    rest = lax.slice_in_dim(values, 0, size - 1, axis=axis)
    border = jnp.zeros_like(lax.slice_in_dim(values, 0, 1, axis=axis))
    return jnp.concatenate([border, rest], axis=axis)

def update_flow(state, upper_plane, delta_time):
    pressure = state[..., 0, :, :, :]
    depth = pressure.ndim
    above = jnp.concatenate([pressure[..., 1:, :, :], upper_plane], axis=depth - 3)
    flow_x = state[..., 1, :, :, :] - delta_time * (shifted_ahead(pressure, depth - 2) - pressure)
    flow_y = state[..., 2, :, :, :] - delta_time * (shifted_ahead(pressure, depth - 1) - pressure)
    flow_z = state[..., 3, :, :, :] - delta_time * (above - pressure)
    return (pressure, flow_x, flow_y, flow_z)

def update_pressure(pressure, flow_x, flow_y, flow_z, lower_plane, speed_sq, delta_time):
    depth = pressure.ndim
    below = jnp.concatenate([lower_plane, flow_z[..., :-1, :, :]], axis=depth - 3)
    diverge = flow_x - shifted_behind(flow_x, depth - 2) + (flow_y - shifted_behind(flow_y, depth - 1)) + (flow_z - below)
    fresh = pressure - delta_time * speed_sq * diverge
    return jnp.stack([fresh, flow_x, flow_y, flow_z], axis=depth - 3)

def advance(state, speed_sq, delta_time):
    zero_plane = jnp.zeros_like(state[..., 0, :1, :, :])
    pressure, flow_x, flow_y, flow_z = update_flow(state, zero_plane, delta_time)
    return update_pressure(pressure, flow_x, flow_y, flow_z, zero_plane, speed_sq, delta_time)

def solve_gram(chol, coef):
    lifted = lax.linalg.triangular_solve(chol, coef[..., None], left_side=True, lower=True)
    solved = lax.linalg.triangular_solve(chol, lifted, left_side=True, lower=True, transpose_a=True)
    return solved[..., 0]

def reference(speed, forcing, guess, basis):
    count = guess.shape[0]
    speed_sq = speed * speed
    loads = forcing.reshape(count, 4, forcing.shape[1], forcing.shape[2], forcing.shape[3])

    def fine_step(state, row_index):
        moved = advance(state, speed_sq, DT)
        return moved.at[:, 0].add(loads[:, row_index])

    def sweep(left):
        points = []
        current = left
        for row_index in range(3):
            current = fine_step(current, row_index)
            points.append(current)
        return points

    def from_left(values):
        return jnp.roll(values, 1, axis=0)
    first_points = sweep(from_left(guess))
    relaxed = fine_step(first_points[-1], 3)
    second_points = sweep(from_left(relaxed))
    residue = fine_step(second_points[-1], 3) - relaxed
    flat_basis = basis.reshape(count, basis.shape[1], -1)

    def build(columns):
        moved = columns
        for repeat in range(4):
            moved = advance(moved, speed_sq, DT)
        return (moved - advance(columns, speed_sq, 4 * DT)).reshape(columns.shape[0], -1)
    corrections = lax.map(build, basis)
    gram = jnp.einsum('krn,ksn->krs', flat_basis, flat_basis, precision=exact_mode)
    chol = jnp.linalg.cholesky(gram)

    def candidate(levels):
        left = from_left(levels)
        moved = advance(left, speed_sq, 4 * DT)
        coef = jnp.einsum('krn,kn->kr', flat_basis, left.reshape(count, -1), precision=exact_mode)
        weights = solve_gram(chol, coef)
        extra = jnp.einsum('kr,krn->kn', weights, corrections, precision=exact_mode).reshape(left.shape)
        return moved + extra + residue
    levels = candidate(residue)
    levels = candidate(levels)
    gap = candidate(levels) - levels
    carry = gap[0:4]
    chained = [carry]
    for group in range(1, count // 4):
        carry = advance(advance(carry, speed_sq, 8 * DT), speed_sq, 8 * DT) + gap[4 * group:4 * group + 4]
        chained.append(carry)
    chain = jnp.concatenate(chained, axis=0)
    levels = candidate(levels + chain)
    final_c = relaxed + levels
    third_points = sweep(from_left(final_c))
    states = jnp.stack(third_points + [final_c], axis=1)
    states = states.reshape(count * 4, 4, guess.shape[2], guess.shape[3], guess.shape[4])
    coef = jnp.einsum('krn,kn->kr', flat_basis, final_c.reshape(count, -1), precision=exact_mode)
    coords = solve_gram(chol, coef)
    return (states, coords)
```

```python
import jax
import jax.numpy as jnp
from jax import lax
from jax.experimental import pallas as pl
from jax.experimental.pallas import tpu as pltpu
from jax.sharding import PartitionSpec as P

DT = 0.045
N_TM = 8
N_SP = 16
RANK = 64
NX = 16
NY = 128
F32 = jnp.float32
BF16 = jnp.bfloat16
VMEM = pl.BlockSpec(memory_space=pltpu.VMEM)
SMEM = pl.BlockSpec(memory_space=pltpu.SMEM)


def hop(value, by_tm, by_space):
    pairs = []
    for k in range(N_TM):
        for s in range(N_SP):
            target = ((k + by_tm) % N_TM) * N_SP + (s + by_space) % N_SP
            pairs.append((k * N_SP + s, target))
    return lax.ppermute(value, ("tm", "space"), pairs)


def share(copies):
    return lax.all_to_all(copies, "space", 0, 0, tiled=True)


def next_x(v):
    row = lax.broadcasted_iota(jnp.int32, v.shape, 1)
    return jnp.where(row < NX - 1, pltpu.roll(v, NX - 1, 1), 0.0)


def prev_x(v):
    row = lax.broadcasted_iota(jnp.int32, v.shape, 1)
    return jnp.where(row > 0, pltpu.roll(v, 1, 1), 0.0)


def next_y(v):
    lane = lax.broadcasted_iota(jnp.int32, v.shape, 2)
    return jnp.where(lane < NY - 1, pltpu.roll(v, NY - 1, 2), 0.0)


def prev_y(v):
    lane = lax.broadcasted_iota(jnp.int32, v.shape, 2)
    return jnp.where(lane > 0, pltpu.roll(v, 1, 2), 0.0)


def cat(*parts):
    parts = [part for part in parts if part.shape[0]]
    return parts[0] if len(parts) == 1 else jnp.concatenate(parts, axis=0)


def only(ok, v):
    return jnp.where(ok, v, jnp.zeros_like(v))


def without_floor(vz, low, ok1, ok2):
    far = max(0, low - 2)
    return cat(only(ok2, vz[:far]), only(ok1, vz[far:low]), vz[low:])


def advance(p, vx, vy, vz, c2, h, low, ok1, ok2, load=None):
    mid = p[1:-1]
    vx = vx - h * (next_x(mid) - mid)
    vy = vy - h * (next_y(mid) - mid)
    vz = vz - h * (p[1:] - p[:-1])
    vz = without_floor(vz, low, ok1, ok2)
    diverge = (vx - prev_x(vx)) + (vy - prev_y(vy)) + (vz[1:] - vz[:-1])
    fresh = mid - h * c2 * diverge
    if load is not None:
        fresh = fresh + load
    return fresh, vx, vy, vz[1:]


def advance_many(p, vx, vy, vz, c2, h, steps, ok1, ok2, loads=None):
    points = []
    for i in range(steps):
        low = steps - i
        load = None if loads is None else loads[i]
        p, vx, vy, vz = advance(p, vx, vy, vz, c2, h, low, ok1, ok2, load)
        edge = low - 1
        n = p.shape[0]
        points.append(
            cat(p[edge : n - edge], vx[edge : n - edge], vy[edge : n - edge], vz[edge : n - edge])
        )
        vx, vy, vz, c2 = vx[1:-1], vy[1:-1], vz[: n - 1], c2[1:-1]
    return points


def put(ref, at, planes):
    n = planes.shape[0]
    ref[at : at + n] = planes
    return at + n


def put_up_far(ref, u, at=0):
    at = put(ref, at, u[0:2])
    at = put(ref, at, u[6:8])
    at = put(ref, at, u[3:4])
    return put(ref, at, u[5:6])


def put_down_far(ref, u, at=0):
    at = put(ref, at, u[0:2])
    at = put(ref, at, u[2:3])
    at = put(ref, at, u[4:5])
    return put(ref, at, u[6:7])


def wide(own, b1, a1, b2, a2, ok_b1, ok_a1, ok_b2, ok_a2):
    p = cat(
        only(ok_b2, b2[0:2]), only(ok_b1, b1[0:2]), own[0:2], only(ok_a1, a1[0:2]), only(ok_a2, a2[0:2])
    )
    vx = cat(b2[4:5], b1[2:4], own[2:4], a1[2:4], a2[2:3])
    vy = cat(b2[5:6], b1[4:6], own[4:6], a1[4:6], a2[3:4])
    vz = cat(b2[2:4], b1[6:8], own[6:8], a1[6:8], a2[4:5])
    return p, vx, vy, vz


def flags(where_ref):
    s = where_ref[0]
    return s >= 1, s < N_SP - 1, s >= 2, s < N_SP - 2


def call(kernel, outs, *args, scratch=(), flops=1_000_000):
    shapes = [jax.ShapeDtypeStruct(shape, F32) for shape in outs]
    return pl.pallas_call(
        kernel,
        out_shape=shapes,
        in_specs=[SMEM if arg.dtype == jnp.int32 else VMEM for arg in args],
        out_specs=[VMEM] * len(shapes),
        scratch_shapes=list(scratch),
        cost_estimate=pl.CostEstimate(flops=flops, bytes_accessed=100_000, transcendentals=0),
    )(*args)


def pack_kernel(g_ref, f_ref, c_ref, up1, dn1, up2, dn2):
    u = g_ref[...]
    c2 = c_ref[...] * c_ref[...]
    for ref, inner in ((up1, 1), (dn1, 0)):
        put(ref, 0, u)
        put(ref, 8, f_ref[0])
        put(ref, 10, f_ref[1])
        put(ref, 12, f_ref[2, inner : inner + 1])
        put(ref, 13, c2)
    at = put_up_far(up2, u)
    at = put(up2, at, f_ref[0, 1:2])
    put(up2, at, c2[1:2])
    at = put_down_far(dn2, u)
    at = put(dn2, at, f_ref[0, 0:1])
    put(dn2, at, c2[0:1])


def load_medium(c_ref, b1, a1, b2, a2, ok):
    ok_b1, ok_a1, ok_b2, ok_a2 = ok
    own = c_ref[...] * c_ref[...]
    return cat(
        only(ok_b2, b2[7:8]), only(ok_b1, b1[13:15]), own, only(ok_a1, a1[13:15]), only(ok_a2, a2[6:7])
    )


def load_forcing(f_ref, b1, a1, b2, a2, ok):
    ok_b1, ok_a1, ok_b2, ok_a2 = ok
    return [
        cat(
            only(ok_b2, b2[6:7]), only(ok_b1, b1[8:10]), f_ref[0], only(ok_a1, a1[8:10]), only(ok_a2, a2[5:6])
        ),
        cat(only(ok_b1, b1[10:12]), f_ref[1], only(ok_a1, a1[10:12])),
        cat(only(ok_b1, b1[12:13]), f_ref[2], only(ok_a1, a1[12:13])),
        f_ref[3],
    ]


def relax_kernel(where, g_ref, f_ref, c_ref, b1, a1, b2, a2, out, up2, dn2):
    ok = flags(where)
    c2 = load_medium(c_ref, b1, a1, b2, a2, ok)
    loads = load_forcing(f_ref, b1, a1, b2, a2, ok)
    p, vx, vy, vz = wide(g_ref[...], b1[...], a1[...], b2[...], a2[...], *ok)
    u = advance_many(p, vx, vy, vz, c2, DT, 4, ok[0], ok[2], loads)[-1]
    out[...] = u
    put_up_far(up2, u)
    put_down_far(dn2, u)


def residue_kernel(where, relaxed, f_ref, c_ref, hb1, ha1, hb2, ha2, own, b1, a1, b2, a2, out, med):
    ok = flags(where)
    c2 = load_medium(c_ref, hb1, ha1, hb2, ha2, ok)
    loads = load_forcing(f_ref, hb1, ha1, hb2, ha2, ok)
    p, vx, vy, vz = wide(own[...], b1[...], a1[...], b2[...], a2[...], *ok)
    u = advance_many(p, vx, vy, vz, c2, DT, 4, ok[0], ok[2], loads)[-1]
    out[...] = u - relaxed[...]
    med[...] = c2


def gram_kernel(basis, out, split):
    rows = 16

    def step(i, total):
        for j in range(rows):
            values = basis[pl.ds(i * rows + j, RANK, stride=8 * NX), :]
            high = values.astype(BF16)
            rest = values - high.astype(F32)
            middle = rest.astype(BF16)
            low = (rest - middle.astype(F32)).astype(BF16)
            lanes = slice(j * NY, (j + 1) * NY)
            split[0:RANK, lanes] = high
            split[RANK : 2 * RANK, lanes] = middle
            split[2 * RANK : 3 * RANK, lanes] = low
        both = split[...]
        return total + lax.dot_general(
            both, both, (((1,), (1,)), ((), ())), preferred_element_type=F32
        )

    total = lax.fori_loop(0, 8 * NX // rows, step, jnp.zeros((3 * RANK, 3 * RANK), F32))
    part = total[0:RANK] + total[RANK : 2 * RANK] + total[2 * RANK :]
    gram = part[:, 0:RANK] + part[:, RANK : 2 * RANK] + part[:, 2 * RANK :]
    out[...] = jnp.concatenate([gram, gram], axis=1)


def inner_products(basis, u, scratch):
    tiles = u.reshape(8 * NX, NY)
    pieces = [tiles[8 * i : 8 * i + 8] for i in range(NX)]
    for r in range(RANK):
        at = r * 8 * NX
        sums = []
        for lane in range(4):
            part = basis[at + 32 * lane : at + 32 * lane + 8, :] * pieces[4 * lane]
            for i in range(1, 4):
                low = at + 32 * lane + 8 * i
                part = part + basis[low : low + 8, :] * pieces[4 * lane + i]
            sums.append(part)
        total = (sums[0] + sums[1]) + (sums[2] + sums[3])
        scratch[r : r + 1, :] = jnp.sum(total, axis=0, keepdims=True)
    column = jnp.sum(scratch[...], axis=1, keepdims=True)
    return to_row(column)


def to_row(column):
    r = lax.broadcasted_iota(jnp.int32, (RANK, NY), 0)
    lane = lax.broadcasted_iota(jnp.int32, (RANK, NY), 1)
    return jnp.sum(jnp.where(r == lane, column, 0.0), axis=0, keepdims=True)


def first_kernel(basis, x_ref, gram, out, scratch):
    row = inner_products(basis, x_ref[...], scratch)
    g = gram[...]
    lane = lax.broadcasted_iota(jnp.int32, (RANK // 2, NY), 1)
    packed = jnp.where(lane < RANK, g[: RANK // 2], g[RANK // 2 :])
    rows = jnp.concatenate([packed, jnp.broadcast_to(row, (8, NY))], axis=0)
    for j in range(N_SP):
        out[j] = rows


def inverse(g):
    lane = lax.broadcasted_iota(jnp.int32, (RANK, NY), 1)
    row = lax.broadcasted_iota(jnp.int32, (RANK, NY), 0)
    work = jnp.where(lane < RANK, g, jnp.where(lane - RANK == row, 1.0, 0.0))
    for j in range(RANK):
        pivot_row = work[j : j + 1, :]
        pivot = work[j : j + 1, j : j + 1]
        scaled = pivot_row * (1.0 / pivot)
        factor = jnp.where(row[:, 0:1] == j, 0.0, work[:, j : j + 1])
        work = work - factor * scaled
    diagonal = jnp.sum(jnp.where(lane == row, work, 0.0), axis=1, keepdims=True)
    solved = pltpu.roll(work, RANK, 1) * (1.0 / diagonal)
    return jnp.where(lane < RANK, solved, 0.0)


def project(basis, ginv, coef, x, scratch, outs):
    weights = jnp.sum(ginv * coef, axis=1, keepdims=True)
    scratch[...] = jnp.broadcast_to(weights, (RANK, NY))
    total = [jnp.zeros((8, NY), F32) for i in range(NX)]
    for r in range(RANK):
        w = scratch[r : r + 1, :]
        at = r * 8 * NX
        for i in range(NX):
            total[i] = total[i] + w * basis[at + 8 * i : at + 8 * i + 8, :]
    y = jnp.concatenate(total, axis=0).reshape(8, NX, NY)
    z = x - y
    center, up1, dn1, up2, dn2 = outs
    put(center, 0, y)
    put(center, 8, z)
    put(up1, 0, y)
    put(up1, 8, z[1:2])
    put(up1, 9, z[7:8])
    put(dn1, 0, y)
    put(dn1, 8, z[0:1])
    put_up_far(up2, y)
    put_down_far(dn2, y)


PROJECTED = [(16, NX, NY), (10, NX, NY), (9, NX, NY), (6, NX, NY), (5, NX, NY)]


def first_project_kernel(got, basis, x_ref, ginv_ref, *rest):
    outs, scratch = rest[:5], rest[5]
    total = got[0]
    for j in range(1, N_SP):
        total = total + got[j]
    packed = total[: RANK // 2]
    g = jnp.concatenate([packed, pltpu.roll(packed, RANK, 1)], axis=0)
    ginv = inverse(g)
    ginv_ref[...] = ginv
    project(basis, ginv, total[RANK // 2 : RANK // 2 + 1], x_ref[...], scratch, outs)


def project_kernel(got, ginv_ref, basis, x_ref, *rest):
    outs, scratch = rest[:5], rest[5]
    coef = jnp.sum(got[...], axis=0)
    project(basis, ginv_ref[...], coef, x_ref[...], scratch, outs)


def q_of(where, med, center, b1, a1, b2, a2):
    ok = flags(where)
    ok_b1, ok_a1 = ok[0], ok[1]
    c2 = med[...]
    y = center[0:8]
    z = center[8:16]
    p, vx, vy, vz = wide(y, b1[...], a1[...], b2[...], a2[...], *ok)
    fine = advance_many(p, vx, vy, vz, c2, DT, 4, ok[0], ok[2])[-1]
    zp = cat(only(ok_b1, b1[8:9]), z[0:2], only(ok_a1, a1[8:9]))
    zz = cat(b1[9:10], z[6:8])
    coarse = advance_many(zp, z[2:4], z[4:6], zz, c2[3:5], 4 * DT, 1, ok[0], ok[2])[-1]
    return fine + coarse


def level_kernel(where, med, center, b1, a1, b2, a2, acc, basis, u_out, acc_out, row_out, scratch):
    u = q_of(where, med, center, b1, a1, b2, a2)
    u_out[...] = u
    acc_out[...] = acc[...] + u
    row = inner_products(basis, u, scratch)
    for j in range(N_SP):
        row_out[j] = row


def gap_kernel(where, med, center, b1, a1, b2, a2, acc, u_out, acc_out, up2, dn2):
    u = q_of(where, med, center, b1, a1, b2, a2)
    u_out[...] = u
    acc_out[...] = acc[...] + u
    put_up_far(up2, u)
    put_down_far(dn2, u)


def chain_kernel(where, med, own, b, a, acc, basis, x_out, row_out, scratch):
    ok = flags(where)
    c2 = med[...]
    p = cat(only(ok[0], b[0:2]), own[0:2], only(ok[1], a[0:2]))
    vx = cat(b[4:5], own[2:4], a[2:3])
    vy = cat(b[5:6], own[4:6], a[3:4])
    vz = cat(b[2:4], own[6:8], a[4:5])
    moved = advance_many(p, vx, vy, vz, c2[2:6], 8 * DT, 2, ok[0], ok[2])[-1]
    chained = (where[1] >= 5) | (where[1] == 0)
    x = acc[...] + only(chained, moved)
    x_out[...] = x
    row = inner_products(basis, x, scratch)
    for j in range(N_SP):
        row_out[j] = row


def final_kernel(where, med, center, b1, a1, b2, a2, relaxed, residue, basis, out, up2, dn2, row_out, scratch):
    u = relaxed[...] + (q_of(where, med, center, b1, a1, b2, a2) + residue[...])
    out[...] = u
    put(up2, put(up2, 0, u[1:2]), u[7:8])
    put(dn2, 0, u[0:1])
    row = inner_products(basis, u, scratch)
    for j in range(N_SP):
        row_out[j] = row


def sweep_kernel(where, f_ref, c_ref, hb1, ha1, hb2, ha2, final, own, b1, a1, b2, a2, got, ginv, out, coords):
    ok = flags(where)
    c2 = load_medium(c_ref, hb1, ha1, hb2, ha2, ok)[1:7]
    loads = [load[1:-1] for load in load_forcing(f_ref, hb1, ha1, hb2, ha2, ok)[:3]]
    u = own[...]
    p = cat(
        only(ok[2], b2[0:1]), only(ok[0], b1[0:2]), u[0:2], only(ok[1], a1[0:2]), only(ok[3], a2[0:1])
    )
    vx = cat(b1[2:4], u[2:4], a1[2:4])
    vy = cat(b1[4:6], u[4:6], a1[4:6])
    vz = cat(b2[1:2], b1[6:8], u[6:8], a1[6:8])
    points = advance_many(p, vx, vy, vz, c2, DT, 3, ok[0], ok[2], loads)
    for i in range(3):
        out[i] = points[i]
    out[3] = final[...]
    coef = jnp.sum(got[...], axis=0)
    coords[...] = to_row(jnp.sum(ginv[...] * coef, axis=1, keepdims=True))


def body(speed, forcing, guess, basis):
    where = jnp.stack([lax.axis_index("space"), lax.axis_index("tm")]).astype(jnp.int32)
    columns = basis.reshape(RANK * 8 * NX, NY)
    state = (8, NX, NY)
    table = pltpu.VMEM((RANK, NY), F32)
    copies = (N_SP, 1, NY)

    start = hop(guess.reshape(state), 1, 0)
    up1, dn1, up2, dn2 = call(
        pack_kernel, [(15, NX, NY), (15, NX, NY), (8, NX, NY), (7, NX, NY)], start, forcing, speed
    )
    halo = (hop(up1, 0, 1), hop(dn1, 0, -1), hop(up2, 0, 2), hop(dn2, 0, -2))
    far = [(6, NX, NY), (5, NX, NY)]
    relaxed, up2, dn2 = call(relax_kernel, [state, *far], where, start, forcing, speed, *halo)
    near = [hop(relaxed, 1, 0), hop(relaxed, 1, 1), hop(relaxed, 1, -1), hop(up2, 1, 2), hop(dn2, 1, -2)]
    (gram,) = call(
        gram_kernel,
        [(RANK, NY)],
        columns,
        scratch=[pltpu.VMEM((3 * RANK, 16 * NY), BF16)],
        flops=50_000_000,
    )
    residue, med = call(
        residue_kernel, [state, (8, NX, NY)], where, relaxed, forcing, speed, *halo, *near
    )
    x = hop(residue, 1, 0)
    (rows,) = call(first_kernel, [(N_SP, RANK // 2 + 8, NY)], columns, x, gram, scratch=[table])
    ginv, *packed = call(
        first_project_kernel, [(RANK, NY), *PROJECTED], share(rows), columns, x, scratch=[table]
    )

    def exchanged(packed, by_tm):
        center, up1, dn1, up2, dn2 = packed
        if by_tm:
            center = hop(center, by_tm, 0)
        return [center, hop(up1, by_tm, 1), hop(dn1, by_tm, -1), hop(up2, by_tm, 2), hop(dn2, by_tm, -2)]

    acc = x
    for level in range(2):
        u, acc, rows = call(
            level_kernel, [state, state, copies], where, med, *exchanged(packed, 1), acc, columns, scratch=[table]
        )
        packed = call(project_kernel, PROJECTED, share(rows), ginv, columns, u, scratch=[table])
    gap, acc, up, dn = call(gap_kernel, [state, state, *far], where, med, *exchanged(packed, 1), acc)
    x, rows = call(
        chain_kernel,
        [state, copies],
        where,
        med,
        hop(gap, 4, 0),
        hop(up, 4, 1),
        hop(dn, 4, -1),
        acc,
        columns,
        scratch=[table],
    )
    packed = call(project_kernel, PROJECTED, share(rows), ginv, columns, x, scratch=[table])
    final, up2, dn2, rows = call(
        final_kernel,
        [state, (2, NX, NY), (1, NX, NY), copies],
        where,
        med,
        *exchanged(packed, 0),
        relaxed,
        residue,
        columns,
        scratch=[table],
    )
    got = share(rows)
    near = [hop(final, 1, 0), hop(final, 1, 1), hop(final, 1, -1)]
    near += [hop(up2, 1, 2), hop(dn2, 1, -2)]
    states, coords = call(
        sweep_kernel, [(4, 8, NX, NY), (1, NY)], where, forcing, speed, *halo, final, *near, got, ginv
    )
    return states.reshape(4, 4, 2, NX, NY), coords[:, :RANK]


def solution(mesh):
    placed = (
        P("space", None, None),
        P("tm", "space", None, None),
        P("tm", None, "space", None, None),
        P("tm", None, None, "space", None, None),
    )
    return jax.shard_map(
        body,
        mesh=mesh,
        in_specs=placed,
        out_specs=(P("tm", None, "space", None, None), P("tm", None)),
        check_vma=False,
    )
```

```python
import jax
import jax.numpy as jnp
from jax import lax
from jax.experimental import pallas as pl
from jax.experimental.pallas import tpu as pltpu
from jax.sharding import PartitionSpec as P

DT = 0.045
N_TM = 8
N_SP = 16
RANK = 64
NX = 16
NY = 128
F32 = jnp.float32
BF16 = jnp.bfloat16
VMEM = pl.BlockSpec(memory_space=pltpu.VMEM)
SMEM = pl.BlockSpec(memory_space=pltpu.SMEM)


def hop(value, by_tm, by_space):
    pairs = []
    for k in range(N_TM):
        for s in range(N_SP):
            target = ((k + by_tm) % N_TM) * N_SP + (s + by_space) % N_SP
            pairs.append((k * N_SP + s, target))
    return lax.ppermute(value, ("tm", "space"), pairs)


def share(copies):
    return lax.all_to_all(copies, "space", 0, 0, tiled=True)


def next_x(v):
    row = lax.broadcasted_iota(jnp.int32, v.shape, 1)
    return jnp.where(row < NX - 1, pltpu.roll(v, NX - 1, 1), 0.0)


def prev_x(v):
    row = lax.broadcasted_iota(jnp.int32, v.shape, 1)
    return jnp.where(row > 0, pltpu.roll(v, 1, 1), 0.0)


def next_y(v):
    lane = lax.broadcasted_iota(jnp.int32, v.shape, 2)
    return jnp.where(lane < NY - 1, pltpu.roll(v, NY - 1, 2), 0.0)


def prev_y(v):
    lane = lax.broadcasted_iota(jnp.int32, v.shape, 2)
    return jnp.where(lane > 0, pltpu.roll(v, 1, 2), 0.0)


def cat(*parts):
    parts = [part for part in parts if part.shape[0]]
    return parts[0] if len(parts) == 1 else jnp.concatenate(parts, axis=0)


def only(ok, v):
    return jnp.where(ok, v, jnp.zeros_like(v))


def without_floor(vz, low, ok1, ok2):
    far = max(0, low - 2)
    return cat(only(ok2, vz[:far]), only(ok1, vz[far:low]), vz[low:])


def advance(p, vx, vy, vz, c2, h, low, ok1, ok2, load=None):
    mid = p[1:-1]
    vx = vx - h * (next_x(mid) - mid)
    vy = vy - h * (next_y(mid) - mid)
    vz = vz - h * (p[1:] - p[:-1])
    vz = without_floor(vz, low, ok1, ok2)
    diverge = (vx - prev_x(vx)) + (vy - prev_y(vy)) + (vz[1:] - vz[:-1])
    fresh = mid - h * c2 * diverge
    if load is not None:
        fresh = fresh + load
    return fresh, vx, vy, vz[1:]


def advance_many(p, vx, vy, vz, c2, h, steps, ok1, ok2, loads=None):
    points = []
    for i in range(steps):
        low = steps - i
        load = None if loads is None else loads[i]
        p, vx, vy, vz = advance(p, vx, vy, vz, c2, h, low, ok1, ok2, load)
        edge = low - 1
        n = p.shape[0]
        points.append(
            cat(p[edge : n - edge], vx[edge : n - edge], vy[edge : n - edge], vz[edge : n - edge])
        )
        vx, vy, vz, c2 = vx[1:-1], vy[1:-1], vz[: n - 1], c2[1:-1]
    return points


def put(ref, at, planes):
    n = planes.shape[0]
    ref[at : at + n] = planes
    return at + n


def put_up_far(ref, u, at=0):
    at = put(ref, at, u[0:2])
    at = put(ref, at, u[6:8])
    at = put(ref, at, u[3:4])
    return put(ref, at, u[5:6])


def put_down_far(ref, u, at=0):
    at = put(ref, at, u[0:2])
    at = put(ref, at, u[2:3])
    at = put(ref, at, u[4:5])
    return put(ref, at, u[6:7])


def wide(own, b1, a1, b2, a2, ok_b1, ok_a1, ok_b2, ok_a2):
    p = cat(
        only(ok_b2, b2[0:2]), only(ok_b1, b1[0:2]), own[0:2], only(ok_a1, a1[0:2]), only(ok_a2, a2[0:2])
    )
    vx = cat(b2[4:5], b1[2:4], own[2:4], a1[2:4], a2[2:3])
    vy = cat(b2[5:6], b1[4:6], own[4:6], a1[4:6], a2[3:4])
    vz = cat(b2[2:4], b1[6:8], own[6:8], a1[6:8], a2[4:5])
    return p, vx, vy, vz


def flags(where_ref):
    s = where_ref[0]
    return s >= 1, s < N_SP - 1, s >= 2, s < N_SP - 2


def call(kernel, outs, *args, scratch=(), flops=1_000_000, limit=4):
    shapes = [pltpu.VMEM(shape, F32) for shape in outs]
    args = [
        arg if arg.dtype == jnp.int32 else pltpu.with_memory_space_constraint(arg, pltpu.VMEM)
        for arg in args
    ]
    return pl.pallas_call(
        kernel,
        out_shape=shapes,
        in_specs=[SMEM if arg.dtype == jnp.int32 else VMEM for arg in args],
        out_specs=[VMEM] * len(shapes),
        scratch_shapes=list(scratch),
        compiler_params=pltpu.CompilerParams(vmem_limit_bytes=limit * 1024 * 1024),
        cost_estimate=pl.CostEstimate(flops=flops, bytes_accessed=100_000, transcendentals=0),
    )(*args)


def pack_kernel(g_ref, f_ref, c_ref, up1, dn1, up2, dn2):
    u = g_ref[...]
    c2 = c_ref[...] * c_ref[...]
    for ref, inner in ((up1, 1), (dn1, 0)):
        put(ref, 0, u)
        put(ref, 8, f_ref[0])
        put(ref, 10, f_ref[1])
        put(ref, 12, f_ref[2, inner : inner + 1])
        put(ref, 13, c2)
    at = put_up_far(up2, u)
    at = put(up2, at, f_ref[0, 1:2])
    put(up2, at, c2[1:2])
    at = put_down_far(dn2, u)
    at = put(dn2, at, f_ref[0, 0:1])
    put(dn2, at, c2[0:1])


def load_medium(c_ref, b1, a1, b2, a2, ok):
    ok_b1, ok_a1, ok_b2, ok_a2 = ok
    own = c_ref[...] * c_ref[...]
    return cat(
        only(ok_b2, b2[7:8]), only(ok_b1, b1[13:15]), own, only(ok_a1, a1[13:15]), only(ok_a2, a2[6:7])
    )


def load_forcing(f_ref, b1, a1, b2, a2, ok):
    ok_b1, ok_a1, ok_b2, ok_a2 = ok
    return [
        cat(
            only(ok_b2, b2[6:7]), only(ok_b1, b1[8:10]), f_ref[0], only(ok_a1, a1[8:10]), only(ok_a2, a2[5:6])
        ),
        cat(only(ok_b1, b1[10:12]), f_ref[1], only(ok_a1, a1[10:12])),
        cat(only(ok_b1, b1[12:13]), f_ref[2], only(ok_a1, a1[12:13])),
        f_ref[3],
    ]


def relax_kernel(where, g_ref, f_ref, c_ref, b1, a1, b2, a2, out, up2, dn2):
    ok = flags(where)
    c2 = load_medium(c_ref, b1, a1, b2, a2, ok)
    loads = load_forcing(f_ref, b1, a1, b2, a2, ok)
    p, vx, vy, vz = wide(g_ref[...], b1[...], a1[...], b2[...], a2[...], *ok)
    u = advance_many(p, vx, vy, vz, c2, DT, 4, ok[0], ok[2], loads)[-1]
    out[...] = u
    put_up_far(up2, u)
    put_down_far(dn2, u)


def residue_kernel(where, relaxed, f_ref, c_ref, hb1, ha1, hb2, ha2, own, b1, a1, b2, a2, out, med):
    ok = flags(where)
    c2 = load_medium(c_ref, hb1, ha1, hb2, ha2, ok)
    loads = load_forcing(f_ref, hb1, ha1, hb2, ha2, ok)
    p, vx, vy, vz = wide(own[...], b1[...], a1[...], b2[...], a2[...], *ok)
    u = advance_many(p, vx, vy, vz, c2, DT, 4, ok[0], ok[2], loads)[-1]
    out[...] = u - relaxed[...]
    med[...] = c2


def gram_kernel(basis, out, split):
    rows = 16

    def step(i, total):
        for j in range(rows):
            values = basis[pl.ds(i * rows + j, RANK, stride=8 * NX), :]
            high = values.astype(BF16)
            rest = values - high.astype(F32)
            middle = rest.astype(BF16)
            low = (rest - middle.astype(F32)).astype(BF16)
            lanes = slice(j * NY, (j + 1) * NY)
            split[0:RANK, lanes] = high
            split[RANK : 2 * RANK, lanes] = middle
            split[2 * RANK : 3 * RANK, lanes] = low
        both = split[...]
        return total + lax.dot_general(
            both, both, (((1,), (1,)), ((), ())), preferred_element_type=F32
        )

    total = lax.fori_loop(0, 8 * NX // rows, step, jnp.zeros((3 * RANK, 3 * RANK), F32))
    part = total[0:RANK] + total[RANK : 2 * RANK] + total[2 * RANK :]
    gram = part[:, 0:RANK] + part[:, RANK : 2 * RANK] + part[:, 2 * RANK :]
    out[...] = jnp.concatenate([gram, gram], axis=1)


def inner_products(basis, u, scratch):
    tiles = u.reshape(8 * NX, NY)
    pieces = [tiles[8 * i : 8 * i + 8] for i in range(NX)]
    for r in range(RANK):
        at = r * 8 * NX
        sums = []
        for lane in range(4):
            part = basis[at + 32 * lane : at + 32 * lane + 8, :] * pieces[4 * lane]
            for i in range(1, 4):
                low = at + 32 * lane + 8 * i
                part = part + basis[low : low + 8, :] * pieces[4 * lane + i]
            sums.append(part)
        total = (sums[0] + sums[1]) + (sums[2] + sums[3])
        scratch[r : r + 1, :] = jnp.sum(total, axis=0, keepdims=True)
    column = jnp.sum(scratch[...], axis=1, keepdims=True)
    return to_row(column)


def to_row(column):
    r = lax.broadcasted_iota(jnp.int32, (RANK, NY), 0)
    lane = lax.broadcasted_iota(jnp.int32, (RANK, NY), 1)
    return jnp.sum(jnp.where(r == lane, column, 0.0), axis=0, keepdims=True)


def first_kernel(basis, x_ref, gram, out, scratch):
    row = inner_products(basis, x_ref[...], scratch)
    g = gram[...]
    lane = lax.broadcasted_iota(jnp.int32, (RANK // 2, NY), 1)
    packed = jnp.where(lane < RANK, g[: RANK // 2], g[RANK // 2 :])
    rows = jnp.concatenate([packed, jnp.broadcast_to(row, (8, NY))], axis=0)
    for j in range(N_SP):
        out[j] = rows


def inverse(g):
    lane = lax.broadcasted_iota(jnp.int32, (RANK, NY), 1)
    row = lax.broadcasted_iota(jnp.int32, (RANK, NY), 0)
    work = jnp.where(lane < RANK, g, jnp.where(lane - RANK == row, 1.0, 0.0))
    for j in range(RANK):
        pivot_row = work[j : j + 1, :]
        pivot = work[j : j + 1, j : j + 1]
        scaled = pivot_row * (1.0 / pivot)
        factor = jnp.where(row[:, 0:1] == j, 0.0, work[:, j : j + 1])
        work = work - factor * scaled
    diagonal = jnp.sum(jnp.where(lane == row, work, 0.0), axis=1, keepdims=True)
    solved = pltpu.roll(work, RANK, 1) * (1.0 / diagonal)
    return jnp.where(lane < RANK, solved, 0.0)


def project(basis, ginv, coef, x, scratch, outs):
    weights = jnp.sum(ginv * coef, axis=1, keepdims=True)
    scratch[...] = jnp.broadcast_to(weights, (RANK, NY))
    total = [jnp.zeros((8, NY), F32) for i in range(NX)]
    for r in range(RANK):
        w = scratch[r : r + 1, :]
        at = r * 8 * NX
        for i in range(NX):
            total[i] = total[i] + w * basis[at + 8 * i : at + 8 * i + 8, :]
    y = jnp.concatenate(total, axis=0).reshape(8, NX, NY)
    z = x - y
    center, up1, dn1, up2, dn2 = outs
    put(center, 0, y)
    put(center, 8, z)
    put(up1, 0, y)
    put(up1, 8, z[1:2])
    put(up1, 9, z[7:8])
    put(dn1, 0, y)
    put(dn1, 8, z[0:1])
    put_up_far(up2, y)
    put_down_far(dn2, y)


PROJECTED = [(16, NX, NY), (10, NX, NY), (9, NX, NY), (6, NX, NY), (5, NX, NY)]


def first_project_kernel(got, basis, x_ref, ginv_ref, *rest):
    outs, scratch = rest[:5], rest[5]
    total = got[0]
    for j in range(1, N_SP):
        total = total + got[j]
    packed = total[: RANK // 2]
    g = jnp.concatenate([packed, pltpu.roll(packed, RANK, 1)], axis=0)
    ginv = inverse(g)
    ginv_ref[...] = ginv
    project(basis, ginv, total[RANK // 2 : RANK // 2 + 1], x_ref[...], scratch, outs)


def project_kernel(got, ginv_ref, basis, x_ref, *rest):
    outs, scratch = rest[:5], rest[5]
    coef = jnp.sum(got[...], axis=0)
    project(basis, ginv_ref[...], coef, x_ref[...], scratch, outs)


def q_of(where, med, center, b1, a1, b2, a2):
    ok = flags(where)
    ok_b1, ok_a1 = ok[0], ok[1]
    c2 = med[...]
    y = center[0:8]
    z = center[8:16]
    p, vx, vy, vz = wide(y, b1[...], a1[...], b2[...], a2[...], *ok)
    fine = advance_many(p, vx, vy, vz, c2, DT, 4, ok[0], ok[2])[-1]
    zp = cat(only(ok_b1, b1[8:9]), z[0:2], only(ok_a1, a1[8:9]))
    zz = cat(b1[9:10], z[6:8])
    coarse = advance_many(zp, z[2:4], z[4:6], zz, c2[3:5], 4 * DT, 1, ok[0], ok[2])[-1]
    return fine + coarse


def level_kernel(where, med, center, b1, a1, b2, a2, acc, basis, u_out, acc_out, row_out, scratch):
    u = q_of(where, med, center, b1, a1, b2, a2)
    u_out[...] = u
    acc_out[...] = acc[...] + u
    row = inner_products(basis, u, scratch)
    for j in range(N_SP):
        row_out[j] = row


def gap_kernel(where, med, center, b1, a1, b2, a2, acc, u_out, acc_out, up2, dn2):
    u = q_of(where, med, center, b1, a1, b2, a2)
    u_out[...] = u
    acc_out[...] = acc[...] + u
    put_up_far(up2, u)
    put_down_far(dn2, u)


def chain_kernel(where, med, own, b, a, acc, basis, x_out, row_out, scratch):
    ok = flags(where)
    c2 = med[...]
    p = cat(only(ok[0], b[0:2]), own[0:2], only(ok[1], a[0:2]))
    vx = cat(b[4:5], own[2:4], a[2:3])
    vy = cat(b[5:6], own[4:6], a[3:4])
    vz = cat(b[2:4], own[6:8], a[4:5])
    moved = advance_many(p, vx, vy, vz, c2[2:6], 8 * DT, 2, ok[0], ok[2])[-1]
    chained = (where[1] >= 5) | (where[1] == 0)
    x = acc[...] + only(chained, moved)
    x_out[...] = x
    row = inner_products(basis, x, scratch)
    for j in range(N_SP):
        row_out[j] = row


def final_kernel(where, med, center, b1, a1, b2, a2, relaxed, residue, basis, out, up2, dn2, row_out, scratch):
    u = relaxed[...] + (q_of(where, med, center, b1, a1, b2, a2) + residue[...])
    out[...] = u
    put(up2, put(up2, 0, u[1:2]), u[7:8])
    put(dn2, 0, u[0:1])
    row = inner_products(basis, u, scratch)
    for j in range(N_SP):
        row_out[j] = row


def sweep_kernel(where, f_ref, c_ref, hb1, ha1, hb2, ha2, final, own, b1, a1, b2, a2, got, ginv, out, coords):
    ok = flags(where)
    c2 = load_medium(c_ref, hb1, ha1, hb2, ha2, ok)[1:7]
    loads = [load[1:-1] for load in load_forcing(f_ref, hb1, ha1, hb2, ha2, ok)[:3]]
    u = own[...]
    p = cat(
        only(ok[2], b2[0:1]), only(ok[0], b1[0:2]), u[0:2], only(ok[1], a1[0:2]), only(ok[3], a2[0:1])
    )
    vx = cat(b1[2:4], u[2:4], a1[2:4])
    vy = cat(b1[4:6], u[4:6], a1[4:6])
    vz = cat(b2[1:2], b1[6:8], u[6:8], a1[6:8])
    points = advance_many(p, vx, vy, vz, c2, DT, 3, ok[0], ok[2], loads)
    for i in range(3):
        out[i] = points[i]
    out[3] = final[...]
    coef = jnp.sum(got[...], axis=0)
    coords[...] = to_row(jnp.sum(ginv[...] * coef, axis=1, keepdims=True))


def body(speed, forcing, guess, basis):
    where = jnp.stack([lax.axis_index("space"), lax.axis_index("tm")]).astype(jnp.int32)
    columns = basis.reshape(RANK * 8 * NX, NY)
    state = (8, NX, NY)
    table = pltpu.VMEM((RANK, NY), F32)
    copies = (N_SP, 1, NY)

    start = hop(guess.reshape(state), 1, 0)
    up1, dn1, up2, dn2 = call(
        pack_kernel, [(15, NX, NY), (15, NX, NY), (8, NX, NY), (7, NX, NY)], start, forcing, speed
    )
    halo = (hop(up1, 0, 1), hop(dn1, 0, -1), hop(up2, 0, 2), hop(dn2, 0, -2))
    far = [(6, NX, NY), (5, NX, NY)]
    relaxed, up2, dn2 = call(relax_kernel, [state, *far], where, start, forcing, speed, *halo)
    near = [hop(relaxed, 1, 0), hop(relaxed, 1, 1), hop(relaxed, 1, -1), hop(up2, 1, 2), hop(dn2, 1, -2)]
    (gram,) = call(
        gram_kernel,
        [(RANK, NY)],
        columns,
        scratch=[pltpu.VMEM((3 * RANK, 16 * NY), BF16)],
        flops=50_000_000,
    )
    residue, med = call(
        residue_kernel, [state, (8, NX, NY)], where, relaxed, forcing, speed, *halo, *near
    )
    x = hop(residue, 1, 0)
    (rows,) = call(first_kernel, [(N_SP, RANK // 2 + 8, NY)], columns, x, gram, scratch=[table])
    ginv, *packed = call(
        first_project_kernel, [(RANK, NY), *PROJECTED], share(rows), columns, x, scratch=[table]
    )

    def exchanged(packed, by_tm):
        center, up1, dn1, up2, dn2 = packed
        if by_tm:
            center = hop(center, by_tm, 0)
        return [center, hop(up1, by_tm, 1), hop(dn1, by_tm, -1), hop(up2, by_tm, 2), hop(dn2, by_tm, -2)]

    acc = x
    for level in range(2):
        u, acc, rows = call(
            level_kernel, [state, state, copies], where, med, *exchanged(packed, 1), acc, columns, scratch=[table]
        )
        packed = call(project_kernel, PROJECTED, share(rows), ginv, columns, u, scratch=[table])
    gap, acc, up, dn = call(gap_kernel, [state, state, *far], where, med, *exchanged(packed, 1), acc)
    x, rows = call(
        chain_kernel,
        [state, copies],
        where,
        med,
        hop(gap, 4, 0),
        hop(up, 4, 1),
        hop(dn, 4, -1),
        acc,
        columns,
        scratch=[table],
    )
    packed = call(project_kernel, PROJECTED, share(rows), ginv, columns, x, scratch=[table])
    final, up2, dn2, rows = call(
        final_kernel,
        [state, (2, NX, NY), (1, NX, NY), copies],
        where,
        med,
        *exchanged(packed, 0),
        relaxed,
        residue,
        columns,
        scratch=[table],
    )
    got = share(rows)
    near = [hop(final, 1, 0), hop(final, 1, 1), hop(final, 1, -1)]
    near += [hop(up2, 1, 2), hop(dn2, 1, -2)]
    states, coords = call(
        sweep_kernel, [(4, 8, NX, NY), (1, NY)], where, forcing, speed, *halo, final, *near, got, ginv
    )
    return states.reshape(4, 4, 2, NX, NY), coords[:, :RANK]


def solution(mesh):
    placed = (
        P("space", None, None),
        P("tm", "space", None, None),
        P("tm", None, "space", None, None),
        P("tm", None, None, "space", None, None),
    )
    return jax.shard_map(
        body,
        mesh=mesh,
        in_specs=placed,
        out_specs=(P("tm", None, "space", None, None), P("tm", None)),
        check_vma=False,
    )
```

```python
import functools

import jax
import jax.numpy as jnp
from jax import lax
from jax.experimental import pallas as pl
from jax.experimental.pallas import tpu as pltpu
from jax.sharding import PartitionSpec as P

DT = 0.045
N_TM = 8
N_SP = 16
RANK = 64
NX = 16
NY = 128
F32 = jnp.float32
BF16 = jnp.bfloat16
VMEM = pl.BlockSpec(memory_space=pltpu.VMEM)
SMEM = pl.BlockSpec(memory_space=pltpu.SMEM)


def moved(value, by_tm, other):
    pairs = []
    for k in range(N_TM):
        for s in range(N_SP):
            slab = other(s)
            if 0 <= slab < N_SP:
                target = ((k + by_tm) % N_TM) * N_SP + slab
            else:
                target = ((k + (by_tm or 1)) % N_TM) * N_SP + s
            pairs.append((k * N_SP + s, target))
    return lax.ppermute(value, ("tm", "space"), pairs)


def hop(value, by_tm):
    return moved(value, by_tm, lambda s: s)


def trade(value, by_tm, step, first):
    low = 0 if first else 1

    def other(s):
        return s + step if (s // step) % 2 == low else s - step

    return moved(value, by_tm, other)


def share(copies):
    return lax.all_to_all(copies, "space", 0, 0, tiled=True)


def next_x(v):
    row = lax.broadcasted_iota(jnp.int32, v.shape, 1)
    return jnp.where(row < NX - 1, pltpu.roll(v, NX - 1, 1), 0.0)


def prev_x(v):
    row = lax.broadcasted_iota(jnp.int32, v.shape, 1)
    return jnp.where(row > 0, pltpu.roll(v, 1, 1), 0.0)


def next_y(v):
    lane = lax.broadcasted_iota(jnp.int32, v.shape, 2)
    return jnp.where(lane < NY - 1, pltpu.roll(v, NY - 1, 2), 0.0)


def prev_y(v):
    lane = lax.broadcasted_iota(jnp.int32, v.shape, 2)
    return jnp.where(lane > 0, pltpu.roll(v, 1, 2), 0.0)


def cat(*parts):
    parts = [part for part in parts if part.shape[0]]
    return parts[0] if len(parts) == 1 else jnp.concatenate(parts, axis=0)


def only(ok, v):
    return jnp.where(ok, v, jnp.zeros_like(v))


def without_floor(vz, low, ok1, ok2):
    far = max(0, low - 2)
    return cat(only(ok2, vz[:far]), only(ok1, vz[far:low]), vz[low:])


def advance_many(p, vx, vy, vz, c2, h, steps, ok1, ok2, loads=None):
    wx, wy = prev_x(vx), prev_y(vy)
    points = []
    for i in range(steps):
        low = steps - i
        mid = p[1:-1]
        row = lax.broadcasted_iota(jnp.int32, mid.shape, 1)
        lane = lax.broadcasted_iota(jnp.int32, mid.shape, 2)
        vx = vx - h * (next_x(mid) - mid)
        vy = vy - h * (next_y(mid) - mid)
        wx = jnp.where(row > 0, wx - h * (mid - pltpu.roll(mid, 1, 1)), 0.0)
        wy = jnp.where(lane > 0, wy - h * (mid - pltpu.roll(mid, 1, 2)), 0.0)
        vz = vz - h * (p[1:] - p[:-1])
        vz = without_floor(vz, low, ok1, ok2)
        diverge = (vx - wx) + (vy - wy) + (vz[1:] - vz[:-1])
        p = mid - h * c2 * diverge
        if loads is not None:
            p = p + loads[i]
        edge = low - 1
        n = p.shape[0]
        own = slice(edge, n - edge)
        points.append(cat(p[own], vx[own], vy[own], vz[1:][own]))
        vx, vy, wx, wy, c2 = (v[1:-1] for v in (vx, vy, wx, wy, c2))
        vz = vz[1:n]
    return points


def put(ref, at, planes):
    n = planes.shape[0]
    ref[at : at + n] = planes
    return at + n


def put_both(refs, up_first, at, both, up=(), down=()):
    first, second = refs
    for planes in both:
        put(first, at, planes)
        at = put(second, at, planes)
    for rising, falling in zip(up, down):
        put(first, at, jnp.where(up_first, rising, falling))
        at = put(second, at, jnp.where(up_first, falling, rising))
    return at


def put_far(refs, up_first, u, more_up=(), more_down=()):
    up = [u[3:4], u[5:6], *more_up]
    down = [u[2:3], u[4:5], *more_down]
    put_both(refs, up_first, 0, [u[0:2], u[6:8]], up, down)


def below_above(up_first, first, second):
    a, b = first[...], second[...]
    return jnp.where(up_first, b, a), jnp.where(up_first, a, b)


def wide(own, b1, a1, b2, a2, ok):
    ok_b1, ok_a1, ok_b2, ok_a2 = ok
    p = cat(
        only(ok_b2, b2[0:2]), only(ok_b1, b1[0:2]), own[0:2], only(ok_a1, a1[0:2]), only(ok_a2, a2[0:2])
    )
    vx = cat(b2[4:5], b1[2:4], own[2:4], a1[2:4], a2[4:5])
    vy = cat(b2[5:6], b1[4:6], own[4:6], a1[4:6], a2[5:6])
    vz = cat(b2[2:4], b1[6:8], own[6:8], a1[6:8], a2[2:3])
    return p, vx, vy, vz


def flags(where_ref):
    s = where_ref[0]
    return s >= 1, s < N_SP - 1, s >= 2, s < N_SP - 2


def ways(where_ref):
    return where_ref[2] == 0, where_ref[3] == 0


def halo_of(where_ref, near, far):
    up1, up2 = ways(where_ref)
    return *below_above(up1, *near), *below_above(up2, *far)


def call(kernel, outs, *args, scratch=(), flops=1_000_000, limit=4):
    shapes = [pltpu.VMEM(shape, F32) for shape in outs]
    args = [
        arg if arg.dtype == jnp.int32 else pltpu.with_memory_space_constraint(arg, pltpu.VMEM)
        for arg in args
    ]
    return pl.pallas_call(
        kernel,
        out_shape=shapes,
        in_specs=[SMEM if arg.dtype == jnp.int32 else VMEM for arg in args],
        out_specs=[VMEM] * len(shapes),
        scratch_shapes=list(scratch),
        compiler_params=pltpu.CompilerParams(vmem_limit_bytes=limit * 1024 * 1024),
        cost_estimate=pl.CostEstimate(flops=flops, bytes_accessed=100_000, transcendentals=0),
    )(*args)


def stage_kernel(f_ref, c_ref, basis, f_out, c2_out):
    f_out[...] = f_ref[...]
    c2_out[...] = c_ref[...] * c_ref[...]


def pack_kernel(where, g_ref, f_ref, c2_ref, e1, o1, e2, o2):
    up1, up2 = ways(where)
    u = g_ref[...]
    c2 = c2_ref[...]
    put_both((e1, o1), up1, 0, [u, f_ref[0], f_ref[1], c2], [f_ref[2, 1:2]], [f_ref[2, 0:1]])
    put_far((e2, o2), up2, u, [f_ref[0, 1:2], c2[1:2]], [f_ref[0, 0:1], c2[0:1]])


def load_medium(own, b1, a1, b2, a2, ok):
    ok_b1, ok_a1, ok_b2, ok_a2 = ok
    return cat(
        only(ok_b2, b2[7:8]), only(ok_b1, b1[12:14]), own, only(ok_a1, a1[12:14]), only(ok_a2, a2[7:8])
    )


def load_forcing(f_ref, b1, a1, b2, a2, ok):
    ok_b1, ok_a1, ok_b2, ok_a2 = ok
    return [
        cat(
            only(ok_b2, b2[6:7]), only(ok_b1, b1[8:10]), f_ref[0], only(ok_a1, a1[8:10]), only(ok_a2, a2[6:7])
        ),
        cat(only(ok_b1, b1[10:12]), f_ref[1], only(ok_a1, a1[10:12])),
        cat(only(ok_b1, b1[14:15]), f_ref[2], only(ok_a1, a1[14:15])),
        f_ref[3],
    ]


LOADS = [8, 6, 4, 2]


def relax_kernel(where, g_ref, f_ref, c2_ref, e1, o1, e2, o2, out, far_e, far_o, med, loads_out):
    ok = flags(where)
    halo = halo_of(where, (e1, o1), (e2, o2))
    c2 = load_medium(c2_ref[...], *halo, ok)
    loads = load_forcing(f_ref, *halo, ok)
    p, vx, vy, vz = wide(g_ref[...], *halo, ok)
    u = advance_many(p, vx, vy, vz, c2, DT, 4, ok[0], ok[2], loads)[-1]
    out[...] = u
    put_far((far_e, far_o), ways(where)[1], u)
    med[...] = c2
    at = 0
    for load in loads:
        at = put(loads_out, at, load)


def kept_loads(loads_ref):
    starts = [sum(LOADS[:i]) for i in range(4)]
    return [loads_ref[start : start + n] for start, n in zip(starts, LOADS)]


def residue_kernel(where, relaxed, loads_ref, med, e2, o2, e1, o1, own, out):
    ok = flags(where)
    p, vx, vy, vz = wide(own[...], *halo_of(where, (e1, o1), (e2, o2)), ok)
    u = advance_many(p, vx, vy, vz, med[...], DT, 4, ok[0], ok[2], kept_loads(loads_ref))[-1]
    out[...] = u - relaxed[...]


def gram_kernel(parts, basis, *refs):
    before = refs[0] if len(refs) == 3 else None
    out, split = refs[-2:]
    rows = 16

    def step(i, total):
        for j in range(rows):
            values = basis[pl.ds(i * rows + j, RANK, stride=8 * NX), :]
            high = values.astype(BF16)
            rest = values - high.astype(F32)
            middle = rest.astype(BF16)
            low = (rest - middle.astype(F32)).astype(BF16)
            lanes = slice(j * NY, (j + 1) * NY)
            split[0:RANK, lanes] = high
            split[RANK : 2 * RANK, lanes] = middle
            split[2 * RANK : 3 * RANK, lanes] = low
        both = split[...]
        return total + lax.dot_general(
            both, both, (((1,), (1,)), ((), ())), preferred_element_type=F32
        )

    total = lax.fori_loop(*parts, step, jnp.zeros((3 * RANK, 3 * RANK), F32))
    part = total[0:RANK] + total[RANK : 2 * RANK] + total[2 * RANK :]
    gram = part[:, 0:RANK] + part[:, RANK : 2 * RANK] + part[:, 2 * RANK :]
    gram = jnp.concatenate([gram, gram], axis=1)
    out[...] = gram if before is None else gram + before[...]


def inner_products(basis, u, scratch):
    tiles = u.reshape(8 * NX, NY)
    pieces = [tiles[8 * i : 8 * i + 8] for i in range(NX)]
    for r in range(RANK):
        at = r * 8 * NX
        sums = []
        for lane in range(4):
            part = basis[at + 32 * lane : at + 32 * lane + 8, :] * pieces[4 * lane]
            for i in range(1, 4):
                low = at + 32 * lane + 8 * i
                part = part + basis[low : low + 8, :] * pieces[4 * lane + i]
            sums.append(part)
        total = (sums[0] + sums[1]) + (sums[2] + sums[3])
        scratch[r : r + 1, :] = jnp.sum(total, axis=0, keepdims=True)
    column = jnp.sum(scratch[...], axis=1, keepdims=True)
    return to_row(column)


def to_row(column):
    r = lax.broadcasted_iota(jnp.int32, (RANK, NY), 0)
    lane = lax.broadcasted_iota(jnp.int32, (RANK, NY), 1)
    return jnp.sum(jnp.where(r == lane, column, 0.0), axis=0, keepdims=True)


def first_kernel(basis, x_ref, gram, out, scratch):
    row = inner_products(basis, x_ref[...], scratch)
    g = gram[...]
    lane = lax.broadcasted_iota(jnp.int32, (RANK // 2, NY), 1)
    packed = jnp.where(lane < RANK, g[: RANK // 2], g[RANK // 2 :])
    rows = jnp.concatenate([packed, jnp.broadcast_to(row, (8, NY))], axis=0)
    for j in range(N_SP):
        out[j] = rows


def inverse(g):
    lane = lax.broadcasted_iota(jnp.int32, (RANK, NY), 1)
    row = lax.broadcasted_iota(jnp.int32, (RANK, NY), 0)
    work = jnp.where(lane < RANK, g, jnp.where(lane - RANK == row, 1.0, 0.0))
    block = 4
    for start in range(0, RANK, block):
        columns = [
            jnp.broadcast_to(work[:, j : j + 1], (RANK, NY)) for j in range(start, start + block)
        ]
        for i in range(block):
            j = start + i
            reciprocal = 1.0 / columns[i][j : j + 1, :]
            factor = jnp.where(row == j, 0.0, columns[i])
            for later in range(i + 1, block):
                scaled = columns[later][j : j + 1, :] * reciprocal
                columns[later] = columns[later] - factor * scaled
            work = work - factor * (work[j : j + 1, :] * reciprocal)
    diagonal = jnp.sum(jnp.where(lane == row, work, 0.0), axis=1, keepdims=True)
    solved = pltpu.roll(work, RANK, 1) * (1.0 / diagonal)
    return jnp.where(lane < RANK, solved, 0.0)


def project(where, basis, ginv, coef, x, scratch, outs):
    weights = jnp.sum(ginv * coef, axis=1, keepdims=True)
    scratch[...] = jnp.broadcast_to(weights, (RANK, NY))
    total = [jnp.zeros((8, NY), F32) for i in range(NX)]
    for r in range(RANK):
        w = scratch[r : r + 1, :]
        at = r * 8 * NX
        for i in range(NX):
            total[i] = total[i] + w * basis[at + 8 * i : at + 8 * i + 8, :]
    y = jnp.concatenate(total, axis=0).reshape(8, NX, NY)
    z = x - y
    center, e1, o1, e2, o2 = outs
    put(center, 0, y)
    put(center, 8, z)
    up1, up2 = ways(where)
    put_both((e1, o1), up1, 0, [y], [z[1:2], z[7:8]], [z[0:1], z[6:7]])
    put_far((e2, o2), up2, y)


PROJECTED = [(16, NX, NY), (10, NX, NY), (10, NX, NY), (6, NX, NY), (6, NX, NY)]


def first_project_kernel(where, got, basis, x_ref, ginv_ref, *rest):
    outs, scratch = rest[:5], rest[5]
    total = got[0]
    for j in range(1, N_SP):
        total = total + got[j]
    packed = total[: RANK // 2]
    g = jnp.concatenate([packed, pltpu.roll(packed, RANK, 1)], axis=0)
    ginv = inverse(g)
    ginv_ref[...] = ginv
    project(where, basis, ginv, total[RANK // 2 : RANK // 2 + 1], x_ref[...], scratch, outs)


def project_kernel(where, got, ginv_ref, basis, x_ref, *rest):
    outs, scratch = rest[:5], rest[5]
    coef = jnp.sum(got[...], axis=0)
    project(where, basis, ginv_ref[...], coef, x_ref[...], scratch, outs)


def q_of(where, med, e2, o2, e1, o1, center):
    ok = flags(where)
    c2 = med[...]
    y = center[0:8]
    z = center[8:16]
    halo = halo_of(where, (e1, o1), (e2, o2))
    b1, a1 = halo[:2]
    p, vx, vy, vz = wide(y, *halo, ok)
    fine = advance_many(p, vx, vy, vz, c2, DT, 4, ok[0], ok[2])[-1]
    zp = cat(only(ok[0], b1[8:9]), z[0:2], only(ok[1], a1[8:9]))
    zz = cat(b1[9:10], z[6:8])
    coarse = advance_many(zp, z[2:4], z[4:6], zz, c2[3:5], 4 * DT, 1, ok[0], ok[2])[-1]
    return fine + coarse


def put_copies(ref, row):
    for j in range(N_SP):
        ref[j] = row


def level_kernel(where, med, e2, o2, e1, o1, center, acc, basis, u_out, acc_out, row_out, scratch):
    u = q_of(where, med, e2, o2, e1, o1, center)
    u_out[...] = u
    acc_out[...] = acc[...] + u
    put_copies(row_out, inner_products(basis, u, scratch))


def gap_kernel(where, med, e2, o2, e1, o1, center, acc, u_out, acc_out, e_out, o_out):
    u = q_of(where, med, e2, o2, e1, o1, center)
    u_out[...] = u
    acc_out[...] = acc[...] + u
    put_far((e_out, o_out), ways(where)[0], u)


def chain_kernel(where, med, o1, e1, own, acc, basis, x_out, row_out, scratch):
    ok = flags(where)
    b, a = below_above(ways(where)[0], e1, o1)
    p = cat(only(ok[0], b[0:2]), own[0:2], only(ok[1], a[0:2]))
    vx = cat(b[4:5], own[2:4], a[4:5])
    vy = cat(b[5:6], own[4:6], a[5:6])
    vz = cat(b[2:4], own[6:8], a[2:3])
    c2 = med[...]
    moved_on = advance_many(p, vx, vy, vz, c2[2:6], 8 * DT, 2, ok[0], ok[2])[-1]
    chained = (where[1] >= 5) | (where[1] == 0)
    x = acc[...] + only(chained, moved_on)
    x_out[...] = x
    put_copies(row_out, inner_products(basis, x, scratch))


def final_kernel(where, med, e2, o2, e1, o1, center, relaxed, residue, basis, out, e_out, o_out, row_out, scratch):
    u = relaxed[...] + (q_of(where, med, e2, o2, e1, o1, center) + residue[...])
    out[...] = u
    up2 = ways(where)[1]
    put_both((e_out, o_out), up2, 0, [], [u[1:2], u[7:8]], [u[0:1], u[6:7]])
    put_copies(row_out, inner_products(basis, u, scratch))


def sweep_kernel(where, loads_ref, med, final, e2, o2, e1, o1, own, got, ginv, out, coords):
    ok = flags(where)
    loads = [load[1:-1] for load in kept_loads(loads_ref)[:3]]
    b1, a1, b2, a2 = halo_of(where, (e1, o1), (e2, o2))
    u = own[...]
    p = cat(
        only(ok[2], b2[0:1]), only(ok[0], b1[0:2]), u[0:2], only(ok[1], a1[0:2]), only(ok[3], a2[0:1])
    )
    vx = cat(b1[2:4], u[2:4], a1[2:4])
    vy = cat(b1[4:6], u[4:6], a1[4:6])
    vz = cat(b2[1:2], b1[6:8], u[6:8], a1[6:8])
    points = advance_many(p, vx, vy, vz, med[1:7], DT, 3, ok[0], ok[2], loads)
    for i in range(3):
        out[i] = points[i]
    out[3] = final[...]
    coef = jnp.sum(got[...], axis=0)
    coords[...] = to_row(jnp.sum(ginv[...] * coef, axis=1, keepdims=True))


def body(speed, forcing, guess, basis):
    slab, block = lax.axis_index("space"), lax.axis_index("tm")
    where = jnp.stack([slab, block, slab % 2, slab // 2 % 2]).astype(jnp.int32)
    columns = basis.reshape(RANK * 8 * NX, NY)
    state = (8, NX, NY)
    table = [pltpu.VMEM((RANK, NY), F32)]
    split = [pltpu.VMEM((3 * RANK, 16 * NY), BF16)]
    copies = (N_SP, 1, NY)
    far = [(6, NX, NY), (6, NX, NY)]

    def traded(near, distant, center, by_tm):
        result = [
            trade(distant[1], by_tm, 2, False),
            trade(distant[0], by_tm, 2, True),
            trade(near[1], by_tm, 1, False),
            trade(near[0], by_tm, 1, True),
        ]
        result = [result[1], result[0], result[3], result[2]]
        return result + ([hop(center, by_tm)] if by_tm else [])

    start = hop(guess.reshape(state), 1)
    load, c2 = call(stage_kernel, [(4, 2, NX, NY), (2, NX, NY)], forcing, speed, columns)
    e1, o1, e2, o2 = call(
        pack_kernel,
        [(15, NX, NY), (15, NX, NY), (8, NX, NY), (8, NX, NY)],
        where,
        start,
        load,
        c2,
    )
    e2, o2, e1, o1 = traded((e1, o1), (e2, o2), None, 0)
    (gram,) = call(
        functools.partial(gram_kernel, (0, 4)), [(RANK, NY)], columns, scratch=split, flops=50_000_000
    )
    relaxed, e, o, med, loads = call(
        relax_kernel,
        [state, *far, (8, NX, NY), (sum(LOADS), NX, NY)],
        where,
        start,
        load,
        c2,
        e1,
        o1,
        e2,
        o2,
    )
    near = traded((relaxed, relaxed), (e, o), relaxed, 1)
    (residue,) = call(residue_kernel, [state], where, relaxed, loads, med, *near)
    x = hop(residue, 1)
    (gram,) = call(
        functools.partial(gram_kernel, (4, 8)), [(RANK, NY)], columns, gram, scratch=split, flops=50_000_000
    )
    (rows,) = call(first_kernel, [(N_SP, RANK // 2 + 8, NY)], columns, x, gram, scratch=table)
    ginv, *packed = call(
        first_project_kernel, [(RANK, NY), *PROJECTED], where, share(rows), columns, x, scratch=table
    )

    def exchanged(packed, by_tm):
        center, e1, o1, e2, o2 = packed
        result = traded((e1, o1), (e2, o2), center, by_tm)
        return result if by_tm else result + [center]

    acc = x
    for level in range(2):
        u, acc, rows = call(
            level_kernel, [state, state, copies], where, med, *exchanged(packed, 1), acc, columns, scratch=table
        )
        packed = call(project_kernel, PROJECTED, where, share(rows), ginv, columns, u, scratch=table)
    gap, acc, e, o = call(gap_kernel, [state, state, *far], where, med, *exchanged(packed, 1), acc)
    o = trade(o, 4, 1, False)
    e = trade(e, 4, 1, True)
    x, rows = call(
        chain_kernel, [state, copies], where, med, o, e, hop(gap, 4), acc, columns, scratch=table
    )
    packed = call(project_kernel, PROJECTED, where, share(rows), ginv, columns, x, scratch=table)
    final, e, o, rows = call(
        final_kernel,
        [state, (2, NX, NY), (2, NX, NY), copies],
        where,
        med,
        *exchanged(packed, 0),
        relaxed,
        residue,
        columns,
        scratch=table,
    )
    got = share(rows)
    near = traded((final, final), (e, o), final, 1)
    states, coords = call(
        sweep_kernel, [(4, 8, NX, NY), (1, NY)], where, loads, med, final, *near, got, ginv
    )
    return states.reshape(4, 4, 2, NX, NY), coords[:, :RANK]


def solution(mesh):
    placed = (
        P("space", None, None),
        P("tm", "space", None, None),
        P("tm", None, "space", None, None),
        P("tm", None, None, "space", None, None),
    )
    return jax.shard_map(
        body,
        mesh=mesh,
        in_specs=placed,
        out_specs=(P("tm", None, "space", None, None), P("tm", None)),
        check_vma=False,
    )
```

```python
import functools

import jax
import jax.numpy as jnp
from jax import lax
from jax.experimental import pallas as pl
from jax.experimental.pallas import tpu as pltpu
from jax.sharding import PartitionSpec as P


DT = 0.045
N_TM = 8
N_SP = 16
RANK = 64
NX = 16
NY = 128
F32 = jnp.float32
BF16 = jnp.bfloat16
VMEM = pl.BlockSpec(memory_space=pltpu.VMEM)


def moved(value, by_tm, other):
    pairs = []
    for k in range(N_TM):
        for s in range(N_SP):
            slab = other(s)
            if 0 <= slab < N_SP:
                target = ((k + by_tm) % N_TM) * N_SP + slab
            else:
                target = ((k + (by_tm or 1)) % N_TM) * N_SP + s
            pairs.append((k * N_SP + s, target))
    return lax.ppermute(value, ("tm", "space"), pairs)


def hop(value, by_tm):
    return moved(value, by_tm, lambda s: s)


def trade(value, by_tm, step, first):
    low = 0 if first else 1

    def other(s):
        return s + step if (s // step) % 2 == low else s - step

    return moved(value, by_tm, other)


def share(copies):
    return lax.all_to_all(copies, "space", 0, 0, tiled=True)


def next_x(v):
    row = lax.broadcasted_iota(jnp.int32, v.shape, 1)
    return jnp.where(row < NX - 1, pltpu.roll(v, NX - 1, 1), 0.0)


def prev_x(v):
    row = lax.broadcasted_iota(jnp.int32, v.shape, 1)
    return jnp.where(row > 0, pltpu.roll(v, 1, 1), 0.0)


def next_y(v):
    lane = lax.broadcasted_iota(jnp.int32, v.shape, 2)
    return jnp.where(lane < NY - 1, pltpu.roll(v, NY - 1, 2), 0.0)


def prev_y(v):
    lane = lax.broadcasted_iota(jnp.int32, v.shape, 2)
    return jnp.where(lane > 0, pltpu.roll(v, 1, 2), 0.0)


def cat(*parts):
    parts = [part for part in parts if part.shape[0]]
    return parts[0] if len(parts) == 1 else jnp.concatenate(parts, axis=0)


def only(ok, v):
    return jnp.where(ok, v, jnp.zeros_like(v))


def without_floor(vz, low, ok1, ok2):
    far = max(0, low - 2)
    return cat(only(ok2, vz[:far]), only(ok1, vz[far:low]), vz[low:])


def advance_many(p, vx, vy, vz, c2, h, steps, ok1, ok2, loads=None):
    wx, wy = prev_x(vx), prev_y(vy)
    points = []
    for i in range(steps):
        low = steps - i
        mid = p[1:-1]
        row = lax.broadcasted_iota(jnp.int32, mid.shape, 1)
        lane = lax.broadcasted_iota(jnp.int32, mid.shape, 2)
        vx = vx - h * (next_x(mid) - mid)
        vy = vy - h * (next_y(mid) - mid)
        wx = jnp.where(row > 0, wx - h * (mid - pltpu.roll(mid, 1, 1)), 0.0)
        wy = jnp.where(lane > 0, wy - h * (mid - pltpu.roll(mid, 1, 2)), 0.0)
        vz = vz - h * (p[1:] - p[:-1])
        vz = without_floor(vz, low, ok1, ok2)
        diverge = (vx - wx) + (vy - wy) + (vz[1:] - vz[:-1])
        p = mid - h * c2 * diverge
        if loads is not None:
            p = p + loads[i]
        edge = low - 1
        n = p.shape[0]
        own = slice(edge, n - edge)
        points.append(cat(p[own], vx[own], vy[own], vz[1:][own]))
        vx, vy, wx, wy, c2 = (v[1:-1] for v in (vx, vy, wx, wy, c2))
        vz = vz[1:n]
    return points


def put(ref, at, planes):
    n = planes.shape[0]
    ref[at : at + n] = planes
    return at + n


def put_both(refs, up_first, at, both, up=(), down=()):
    first, second = refs
    for planes in both:
        put(first, at, planes)
        at = put(second, at, planes)
    for rising, falling in zip(up, down):
        put(first, at, jnp.where(up_first, rising, falling))
        at = put(second, at, jnp.where(up_first, falling, rising))
    return at


def put_far(refs, up_first, u, more_up=(), more_down=()):
    up = [u[3:4], u[5:6], *more_up]
    down = [u[2:3], u[4:5], *more_down]
    put_both(refs, up_first, 0, [u[0:2], u[6:8]], up, down)


def below_above(up_first, first, second):
    a, b = first[...], second[...]
    return jnp.where(up_first, b, a), jnp.where(up_first, a, b)


def wide(own, b1, a1, b2, a2, ok):
    ok_b1, ok_a1, ok_b2, ok_a2 = ok
    p = cat(
        only(ok_b2, b2[0:2]), only(ok_b1, b1[0:2]), own[0:2], only(ok_a1, a1[0:2]), only(ok_a2, a2[0:2])
    )
    vx = cat(b2[4:5], b1[2:4], own[2:4], a1[2:4], a2[4:5])
    vy = cat(b2[5:6], b1[4:6], own[4:6], a1[4:6], a2[5:6])
    vz = cat(b2[2:4], b1[6:8], own[6:8], a1[6:8], a2[2:3])
    return p, vx, vy, vz


def flags():
    s = lax.axis_index("space")
    return s >= 1, s < N_SP - 1, s >= 2, s < N_SP - 2


def ways():
    s = lax.axis_index("space")
    return (s & 1) == 0, (s & 2) == 0


def halo_of(near, far):
    up1, up2 = ways()
    return *below_above(up1, *near), *below_above(up2, *far)


def call(kernel, outs, *args, scratch=(), flops=1_000_000, limit=4, outward=False):
    kind = pltpu.HBM if outward else pltpu.VMEM
    shapes = [kind(shape, F32) for shape in outs]
    args = [pltpu.with_memory_space_constraint(arg, pltpu.VMEM) for arg in args]
    return pl.pallas_call(
        kernel,
        out_shape=shapes,
        in_specs=[VMEM] * len(args),
        out_specs=[pl.BlockSpec(memory_space=kind)] * len(shapes),
        scratch_shapes=list(scratch),
        compiler_params=pltpu.CompilerParams(vmem_limit_bytes=limit * 1024 * 1024),
        cost_estimate=pl.CostEstimate(flops=flops, bytes_accessed=100_000, transcendentals=0),
    )(*args)


def stage_kernel(f_ref, c_ref, basis, f_out, c2_out):
    f_out[...] = f_ref[...]
    c2_out[...] = c_ref[...] * c_ref[...]


def pack_kernel(g_ref, f_ref, c2_ref, e1, o1, e2, o2):
    up1, up2 = ways()
    u = g_ref[...]
    c2 = c2_ref[...]
    put_both((e1, o1), up1, 0, [u, f_ref[0], f_ref[1], c2], [f_ref[2, 1:2]], [f_ref[2, 0:1]])
    put_far((e2, o2), up2, u, [f_ref[0, 1:2], c2[1:2]], [f_ref[0, 0:1], c2[0:1]])


def load_medium(own, b1, a1, b2, a2, ok):
    ok_b1, ok_a1, ok_b2, ok_a2 = ok
    return cat(
        only(ok_b2, b2[7:8]), only(ok_b1, b1[12:14]), own, only(ok_a1, a1[12:14]), only(ok_a2, a2[7:8])
    )


def load_forcing(f_ref, b1, a1, b2, a2, ok):
    ok_b1, ok_a1, ok_b2, ok_a2 = ok
    return [
        cat(
            only(ok_b2, b2[6:7]), only(ok_b1, b1[8:10]), f_ref[0], only(ok_a1, a1[8:10]), only(ok_a2, a2[6:7])
        ),
        cat(only(ok_b1, b1[10:12]), f_ref[1], only(ok_a1, a1[10:12])),
        cat(only(ok_b1, b1[14:15]), f_ref[2], only(ok_a1, a1[14:15])),
        f_ref[3],
    ]


LOADS = [8, 6, 4, 2]


def relax_kernel(g_ref, f_ref, c2_ref, e1, o1, e2, o2, out, far_e, far_o, med, loads_out):
    ok = flags()
    halo = halo_of((e1, o1), (e2, o2))
    c2 = load_medium(c2_ref[...], *halo, ok)
    loads = load_forcing(f_ref, *halo, ok)
    p, vx, vy, vz = wide(g_ref[...], *halo, ok)
    u = advance_many(p, vx, vy, vz, c2, DT, 4, ok[0], ok[2], loads)[-1]
    out[...] = u
    put_far((far_e, far_o), ways()[1], u)
    med[...] = c2
    at = 0
    for load in loads:
        at = put(loads_out, at, load)


def kept_loads(loads_ref):
    starts = [sum(LOADS[:i]) for i in range(4)]
    return [loads_ref[start : start + n] for start, n in zip(starts, LOADS)]


def residue_kernel(relaxed, loads_ref, med, e2, o2, e1, o1, own, out):
    ok = flags()
    p, vx, vy, vz = wide(own[...], *halo_of((e1, o1), (e2, o2)), ok)
    u = advance_many(p, vx, vy, vz, med[...], DT, 4, ok[0], ok[2], kept_loads(loads_ref))[-1]
    out[...] = u - relaxed[...]


def gram_kernel(parts, basis, *refs):
    before = refs[0] if len(refs) == 3 else None
    out, split = refs[-2:]
    rows = 16

    def step(i, total):
        for j in range(rows):
            values = basis[pl.ds(i * rows + j, RANK, stride=8 * NX), :]
            high = values.astype(BF16)
            rest = values - high.astype(F32)
            middle = rest.astype(BF16)
            low = (rest - middle.astype(F32)).astype(BF16)
            lanes = slice(j * NY, (j + 1) * NY)
            split[0:RANK, lanes] = high
            split[RANK : 2 * RANK, lanes] = middle
            split[2 * RANK : 3 * RANK, lanes] = low
        both = split[...]
        return total + lax.dot_general(
            both, both, (((1,), (1,)), ((), ())), preferred_element_type=F32
        )

    total = lax.fori_loop(*parts, step, jnp.zeros((3 * RANK, 3 * RANK), F32))
    part = total[0:RANK] + total[RANK : 2 * RANK] + total[2 * RANK :]
    gram = part[:, 0:RANK] + part[:, RANK : 2 * RANK] + part[:, 2 * RANK :]
    gram = jnp.concatenate([gram, gram], axis=1)
    out[...] = gram if before is None else gram + before[...]


def inner_products(basis, u, scratch):
    tiles = u.reshape(8 * NX, NY)
    pieces = [tiles[8 * i : 8 * i + 8] for i in range(NX)]
    for r in range(RANK):
        at = r * 8 * NX
        sums = []
        for lane in range(4):
            part = basis[at + 32 * lane : at + 32 * lane + 8, :] * pieces[4 * lane]
            for i in range(1, 4):
                low = at + 32 * lane + 8 * i
                part = part + basis[low : low + 8, :] * pieces[4 * lane + i]
            sums.append(part)
        total = (sums[0] + sums[1]) + (sums[2] + sums[3])
        scratch[r : r + 1, :] = jnp.sum(total, axis=0, keepdims=True)
    column = jnp.sum(scratch[...], axis=1, keepdims=True)
    return to_row(column)


def to_row(column):
    r = lax.broadcasted_iota(jnp.int32, (RANK, NY), 0)
    lane = lax.broadcasted_iota(jnp.int32, (RANK, NY), 1)
    return jnp.sum(jnp.where(r == lane, column, 0.0), axis=0, keepdims=True)


def first_kernel(basis, x_ref, gram, out, scratch):
    row = inner_products(basis, x_ref[...], scratch)
    g = gram[...]
    lane = lax.broadcasted_iota(jnp.int32, (RANK // 2, NY), 1)
    packed = jnp.where(lane < RANK, g[: RANK // 2], g[RANK // 2 :])
    rows = jnp.concatenate([packed, jnp.broadcast_to(row, (8, NY))], axis=0)
    for j in range(N_SP):
        out[j] = rows


def inverse(g):
    lane = lax.broadcasted_iota(jnp.int32, (RANK, NY), 1)
    row = lax.broadcasted_iota(jnp.int32, (RANK, NY), 0)
    work = jnp.where(lane < RANK, g, jnp.where(lane - RANK == row, 1.0, 0.0))
    block = 4
    for start in range(0, RANK, block):
        columns = [
            jnp.broadcast_to(work[:, j : j + 1], (RANK, NY)) for j in range(start, start + block)
        ]
        for i in range(block):
            j = start + i
            reciprocal = 1.0 / columns[i][j : j + 1, :]
            factor = jnp.where(row == j, 0.0, columns[i])
            for later in range(i + 1, block):
                scaled = columns[later][j : j + 1, :] * reciprocal
                columns[later] = columns[later] - factor * scaled
            work = work - factor * (work[j : j + 1, :] * reciprocal)
    diagonal = jnp.sum(jnp.where(lane == row, work, 0.0), axis=1, keepdims=True)
    solved = pltpu.roll(work, RANK, 1) * (1.0 / diagonal)
    return jnp.where(lane < RANK, solved, 0.0)


def project(basis, ginv, coef, x, scratch, outs):
    weights = jnp.sum(ginv * coef, axis=1, keepdims=True)
    scratch[...] = jnp.broadcast_to(weights, (RANK, NY))
    total = [jnp.zeros((8, NY), F32) for _ in range(NX)]
    for r in range(RANK):
        w = scratch[r : r + 1, :]
        at = r * 8 * NX
        for i in range(NX):
            total[i] = total[i] + w * basis[at + 8 * i : at + 8 * i + 8, :]
    y = jnp.concatenate(total, axis=0).reshape(8, NX, NY)
    z = x - y
    center, e1, o1, e2, o2 = outs
    put(center, 0, y)
    put(center, 8, z)
    up1, up2 = ways()
    put_both((e1, o1), up1, 0, [y], [z[1:2], z[7:8]], [z[0:1], z[6:7]])
    put_far((e2, o2), up2, y)


PROJECTED = [(16, NX, NY), (10, NX, NY), (10, NX, NY), (6, NX, NY), (6, NX, NY)]


def first_project_kernel(got, basis, x_ref, ginv_ref, *rest):
    outs, scratch = rest[:5], rest[5]
    total = got[0]
    for j in range(1, N_SP):
        total = total + got[j]
    packed = total[: RANK // 2]
    g = jnp.concatenate([packed, pltpu.roll(packed, RANK, 1)], axis=0)
    ginv = inverse(g)
    ginv_ref[...] = ginv
    project(basis, ginv, total[RANK // 2 : RANK // 2 + 1], x_ref[...], scratch, outs)


def project_kernel(got, ginv_ref, basis, x_ref, *rest):
    outs, scratch = rest[:5], rest[5]
    coef = jnp.sum(got[...], axis=0)
    project(basis, ginv_ref[...], coef, x_ref[...], scratch, outs)


def q_of(med, e2, o2, e1, o1, center):
    ok = flags()
    c2 = med[...]
    y = center[0:8]
    z = center[8:16]
    halo = halo_of((e1, o1), (e2, o2))
    b1, a1 = halo[:2]
    p, vx, vy, vz = wide(y, *halo, ok)
    fine = advance_many(p, vx, vy, vz, c2, DT, 4, ok[0], ok[2])[-1]
    zp = cat(only(ok[0], b1[8:9]), z[0:2], only(ok[1], a1[8:9]))
    zz = cat(b1[9:10], z[6:8])
    coarse = advance_many(zp, z[2:4], z[4:6], zz, c2[3:5], 4 * DT, 1, ok[0], ok[2])[-1]
    return fine + coarse


def put_copies(ref, row):
    for j in range(N_SP):
        ref[j] = row


def level_kernel(med, e2, o2, e1, o1, center, acc, basis, u_out, acc_out, row_out, scratch):
    u = q_of(med, e2, o2, e1, o1, center)
    u_out[...] = u
    acc_out[...] = acc[...] + u
    put_copies(row_out, inner_products(basis, u, scratch))


def gap_kernel(med, e2, o2, e1, o1, center, acc, u_out, acc_out, e_out, o_out):
    u = q_of(med, e2, o2, e1, o1, center)
    u_out[...] = u
    acc_out[...] = acc[...] + u
    put_far((e_out, o_out), ways()[0], u)


def chain_kernel(med, o1, e1, own, acc, basis, x_out, row_out, scratch):
    ok = flags()
    b, a = below_above(ways()[0], e1, o1)
    p = cat(only(ok[0], b[0:2]), own[0:2], only(ok[1], a[0:2]))
    vx = cat(b[4:5], own[2:4], a[4:5])
    vy = cat(b[5:6], own[4:6], a[5:6])
    vz = cat(b[2:4], own[6:8], a[2:3])
    c2 = med[...]
    moved_on = advance_many(p, vx, vy, vz, c2[2:6], 8 * DT, 2, ok[0], ok[2])[-1]
    row = lax.axis_index("tm")
    chained = (row >= 5) | (row == 0)
    x = acc[...] + only(chained, moved_on)
    x_out[...] = x
    put_copies(row_out, inner_products(basis, x, scratch))


def final_kernel(med, e2, o2, e1, o1, center, relaxed, residue, basis, out, e_out, o_out, row_out, scratch):
    u = relaxed[...] + (q_of(med, e2, o2, e1, o1, center) + residue[...])
    out[...] = u
    up2 = ways()[1]
    put_both((e_out, o_out), up2, 0, [], [u[1:2], u[7:8]], [u[0:1], u[6:7]])
    put_copies(row_out, inner_products(basis, u, scratch))


def sweep_kernel(loads_ref, med, final, e2, o2, e1, o1, own, got, ginv, out, coords, kept, kept_row, sems):
    def copy(row, source):
        return pltpu.make_async_copy(source, out.at[row], sems.at[row])

    copies = [copy(3, final)]
    copies[0].start()
    coef = jnp.sum(got[...], axis=0)
    kept_row[...] = to_row(jnp.sum(ginv[...] * coef, axis=1, keepdims=True))
    copies.append(pltpu.make_async_copy(kept_row, coords, sems.at[4]))
    copies[1].start()
    ok = flags()
    loads = [load[1:-1] for load in kept_loads(loads_ref)[:3]]
    b1, a1, b2, a2 = halo_of((e1, o1), (e2, o2))
    u = own[...]
    p = cat(
        only(ok[2], b2[0:1]), only(ok[0], b1[0:2]), u[0:2], only(ok[1], a1[0:2]), only(ok[3], a2[0:1])
    )
    vx = cat(b1[2:4], u[2:4], a1[2:4])
    vy = cat(b1[4:6], u[4:6], a1[4:6])
    vz = cat(b2[1:2], b1[6:8], u[6:8], a1[6:8])
    points = advance_many(p, vx, vy, vz, med[1:7], DT, 3, ok[0], ok[2], loads)
    for i in range(3):
        kept[i] = points[i]
        copies.append(copy(i, kept.at[i]))
        copies[-1].start()
    for each in copies:
        each.wait()


def body(speed, forcing, guess, basis):
    columns = basis.reshape(RANK * 8 * NX, NY)
    state = (8, NX, NY)
    table = [pltpu.VMEM((RANK, NY), F32)]
    split = [pltpu.VMEM((3 * RANK, 16 * NY), BF16)]
    copies = (N_SP, 1, NY)
    far = [(6, NX, NY), (6, NX, NY)]

    def traded(near, distant, center, by_tm):
        far_second = trade(distant[1], by_tm, 2, False)
        far_first = trade(distant[0], by_tm, 2, True)
        near_second = trade(near[1], by_tm, 1, False)
        near_first = trade(near[0], by_tm, 1, True)
        result = [far_first, far_second, near_first, near_second]
        if by_tm:
            result.append(hop(center, by_tm))
        return result

    start = hop(guess.reshape(state), 1)
    load, c2 = call(stage_kernel, [(4, 2, NX, NY), (2, NX, NY)], forcing, speed, columns)
    e1, o1, e2, o2 = call(
        pack_kernel,
        [(15, NX, NY), (15, NX, NY), (8, NX, NY), (8, NX, NY)],
        start,
        load,
        c2,
    )
    e2, o2, e1, o1 = traded((e1, o1), (e2, o2), None, 0)
    (gram,) = call(
        functools.partial(gram_kernel, (0, 4)), [(RANK, NY)], columns, scratch=split, flops=50_000_000
    )
    relaxed, e, o, med, loads = call(
        relax_kernel,
        [state, *far, (8, NX, NY), (sum(LOADS), NX, NY)],
        start,
        load,
        c2,
        e1,
        o1,
        e2,
        o2,
    )
    near = traded((relaxed, relaxed), (e, o), relaxed, 1)
    (residue,) = call(residue_kernel, [state], relaxed, loads, med, *near)
    x = hop(residue, 1)
    (gram,) = call(
        functools.partial(gram_kernel, (4, 8)), [(RANK, NY)], columns, gram, scratch=split, flops=50_000_000
    )
    (rows,) = call(first_kernel, [(N_SP, RANK // 2 + 8, NY)], columns, x, gram, scratch=table)
    ginv, *packed = call(
        first_project_kernel, [(RANK, NY), *PROJECTED], share(rows), columns, x, scratch=table
    )

    def exchanged(packed, by_tm):
        center, e1, o1, e2, o2 = packed
        result = traded((e1, o1), (e2, o2), center, by_tm)
        return result if by_tm else result + [center]

    acc = x
    for _ in range(2):
        u, acc, rows = call(
            level_kernel, [state, state, copies], med, *exchanged(packed, 1), acc, columns, scratch=table
        )
        packed = call(project_kernel, PROJECTED, share(rows), ginv, columns, u, scratch=table)
    gap, acc, e, o = call(gap_kernel, [state, state, *far], med, *exchanged(packed, 1), acc)
    o = trade(o, 4, 1, False)
    e = trade(e, 4, 1, True)
    x, rows = call(
        chain_kernel, [state, copies], med, o, e, hop(gap, 4), acc, columns, scratch=table
    )
    packed = call(project_kernel, PROJECTED, share(rows), ginv, columns, x, scratch=table)
    final, e, o, rows = call(
        final_kernel,
        [state, (2, NX, NY), (2, NX, NY), copies],
        med,
        *exchanged(packed, 0),
        relaxed,
        residue,
        columns,
        scratch=table,
    )
    got = share(rows)
    near = traded((final, final), (e, o), final, 1)
    states, coords = call(
        sweep_kernel,
        [(4, 8, NX, NY), (1, NY)],
        loads,
        med,
        final,
        *near,
        got,
        ginv,
        scratch=[pltpu.VMEM((3, 8, NX, NY), F32), pltpu.VMEM((1, NY), F32), pltpu.SemaphoreType.DMA((5,))],
        outward=True,
    )
    return states.reshape(4, 4, 2, NX, NY), coords[:, :RANK]


def solution(mesh):
    placed = (
        P("space", None, None),
        P("tm", "space", None, None),
        P("tm", None, "space", None, None),
        P("tm", None, None, "space", None, None),
    )
    return jax.shard_map(
        body,
        mesh=mesh,
        in_specs=placed,
        out_specs=(P("tm", None, "space", None, None), P("tm", None)),
        check_vma=False,
    )
```

```python
import functools

import jax
import jax.numpy as jnp
from jax import lax
from jax.experimental import pallas as pl
from jax.experimental.pallas import tpu as pltpu
from jax.sharding import PartitionSpec as P


DT = 0.045
N_TM = 8
N_SP = 16
RANK = 64
NX = 16
NY = 128
F32 = jnp.float32
BF16 = jnp.bfloat16
VMEM = pl.BlockSpec(memory_space=pltpu.VMEM)


def moved(value, by_tm, other):
    pairs = []
    for k in range(N_TM):
        for s in range(N_SP):
            slab = other(s)
            if 0 <= slab < N_SP:
                target = ((k + by_tm) % N_TM) * N_SP + slab
            else:
                target = ((k + (by_tm or 1)) % N_TM) * N_SP + s
            pairs.append((k * N_SP + s, target))
    return lax.ppermute(value, ("tm", "space"), pairs)


def hop(value, by_tm):
    return moved(value, by_tm, lambda s: s)


def trade(value, by_tm, step, first):
    low = 0 if first else 1

    def other(s):
        return s + step if (s // step) % 2 == low else s - step

    return moved(value, by_tm, other)


def share(copies):
    return lax.all_to_all(copies, "space", 0, 0, tiled=True)


def next_x(v):
    row = lax.broadcasted_iota(jnp.int32, v.shape, 1)
    return jnp.where(row < NX - 1, pltpu.roll(v, NX - 1, 1), 0.0)


def prev_x(v):
    row = lax.broadcasted_iota(jnp.int32, v.shape, 1)
    return jnp.where(row > 0, pltpu.roll(v, 1, 1), 0.0)


def next_y(v):
    lane = lax.broadcasted_iota(jnp.int32, v.shape, 2)
    return jnp.where(lane < NY - 1, pltpu.roll(v, NY - 1, 2), 0.0)


def prev_y(v):
    lane = lax.broadcasted_iota(jnp.int32, v.shape, 2)
    return jnp.where(lane > 0, pltpu.roll(v, 1, 2), 0.0)


def cat(*parts):
    parts = [part for part in parts if part.shape[0]]
    return parts[0] if len(parts) == 1 else jnp.concatenate(parts, axis=0)


def only(ok, v):
    return jnp.where(ok, v, jnp.zeros_like(v))


def without_floor(vz, low, ok1, ok2):
    far = max(0, low - 2)
    return cat(only(ok2, vz[:far]), only(ok1, vz[far:low]), vz[low:])


def advance_many(p, vx, vy, vz, c2, h, steps, ok1, ok2, loads=None):
    wx, wy = prev_x(vx), prev_y(vy)
    points = []
    for i in range(steps):
        low = steps - i
        mid = p[1:-1]
        row = lax.broadcasted_iota(jnp.int32, mid.shape, 1)
        lane = lax.broadcasted_iota(jnp.int32, mid.shape, 2)
        vx = vx - h * (next_x(mid) - mid)
        vy = vy - h * (next_y(mid) - mid)
        wx = jnp.where(row > 0, wx - h * (mid - pltpu.roll(mid, 1, 1)), 0.0)
        wy = jnp.where(lane > 0, wy - h * (mid - pltpu.roll(mid, 1, 2)), 0.0)
        vz = vz - h * (p[1:] - p[:-1])
        vz = without_floor(vz, low, ok1, ok2)
        diverge = (vx - wx) + (vy - wy) + (vz[1:] - vz[:-1])
        p = mid - h * c2 * diverge
        if loads is not None:
            p = p + loads[i]
        edge = low - 1
        n = p.shape[0]
        own = slice(edge, n - edge)
        points.append(cat(p[own], vx[own], vy[own], vz[1:][own]))
        vx, vy, wx, wy, c2 = (v[1:-1] for v in (vx, vy, wx, wy, c2))
        vz = vz[1:n]
    return points


def put(ref, at, planes):
    n = planes.shape[0]
    ref[at : at + n] = planes
    return at + n


def put_both(refs, up_first, at, both, up=(), down=()):
    first, second = refs
    for planes in both:
        put(first, at, planes)
        at = put(second, at, planes)
    for rising, falling in zip(up, down):
        put(first, at, jnp.where(up_first, rising, falling))
        at = put(second, at, jnp.where(up_first, falling, rising))
    return at


def put_far(refs, up_first, u, more_up=(), more_down=()):
    up = [u[3:4], u[5:6], *more_up]
    down = [u[2:3], u[4:5], *more_down]
    put_both(refs, up_first, 0, [u[0:2], u[6:8]], up, down)


def below_above(up_first, first, second):
    a, b = first[...], second[...]
    return jnp.where(up_first, b, a), jnp.where(up_first, a, b)


def wide(own, b1, a1, b2, a2, ok):
    ok_b1, ok_a1, ok_b2, ok_a2 = ok
    p = cat(
        only(ok_b2, b2[0:2]), only(ok_b1, b1[0:2]), own[0:2], only(ok_a1, a1[0:2]), only(ok_a2, a2[0:2])
    )
    vx = cat(b2[4:5], b1[2:4], own[2:4], a1[2:4], a2[4:5])
    vy = cat(b2[5:6], b1[4:6], own[4:6], a1[4:6], a2[5:6])
    vz = cat(b2[2:4], b1[6:8], own[6:8], a1[6:8], a2[2:3])
    return p, vx, vy, vz


def flags():
    s = lax.axis_index("space")
    return s >= 1, s < N_SP - 1, s >= 2, s < N_SP - 2


def ways():
    s = lax.axis_index("space")
    return (s & 1) == 0, (s & 2) == 0


def halo_of(near, far):
    up1, up2 = ways()
    return *below_above(up1, *near), *below_above(up2, *far)


def call(kernel, outs, *args, scratch=(), flops=1_000_000, limit=4, outward=False):
    kind = pltpu.HBM if outward else pltpu.VMEM
    shapes = [kind(shape, F32) for shape in outs]
    args = [pltpu.with_memory_space_constraint(arg, pltpu.VMEM) for arg in args]
    return pl.pallas_call(
        kernel,
        out_shape=shapes,
        in_specs=[VMEM] * len(args),
        out_specs=[pl.BlockSpec(memory_space=kind)] * len(shapes),
        scratch_shapes=list(scratch),
        compiler_params=pltpu.CompilerParams(vmem_limit_bytes=limit * 1024 * 1024),
        cost_estimate=pl.CostEstimate(flops=flops, bytes_accessed=100_000, transcendentals=0),
    )(*args)


def stage_kernel(c_ref, basis, c2_out):
    c2_out[...] = c_ref[...] * c_ref[...]


def pack_kernel(g_ref, f_ref, c2_ref, e1, o1, e2, o2):
    up1, up2 = ways()
    u = g_ref[...]
    c2 = c2_ref[...]
    put_both((e1, o1), up1, 0, [u, f_ref[0], f_ref[1], c2], [f_ref[2, 1:2]], [f_ref[2, 0:1]])
    put_far((e2, o2), up2, u, [f_ref[0, 1:2], c2[1:2]], [f_ref[0, 0:1], c2[0:1]])


def load_medium(own, b1, a1, b2, a2, ok):
    ok_b1, ok_a1, ok_b2, ok_a2 = ok
    return cat(
        only(ok_b2, b2[7:8]), only(ok_b1, b1[12:14]), own, only(ok_a1, a1[12:14]), only(ok_a2, a2[7:8])
    )


def load_forcing(f_ref, b1, a1, b2, a2, ok):
    ok_b1, ok_a1, ok_b2, ok_a2 = ok
    return [
        cat(
            only(ok_b2, b2[6:7]), only(ok_b1, b1[8:10]), f_ref[0], only(ok_a1, a1[8:10]), only(ok_a2, a2[6:7])
        ),
        cat(only(ok_b1, b1[10:12]), f_ref[1], only(ok_a1, a1[10:12])),
        cat(only(ok_b1, b1[14:15]), f_ref[2], only(ok_a1, a1[14:15])),
        f_ref[3],
    ]


LOADS = [8, 6, 4, 2]


def relax_kernel(g_ref, f_ref, c2_ref, e1, o1, e2, o2, out, far_e, far_o, med, loads_out):
    ok = flags()
    halo = halo_of((e1, o1), (e2, o2))
    c2 = load_medium(c2_ref[...], *halo, ok)
    loads = load_forcing(f_ref, *halo, ok)
    p, vx, vy, vz = wide(g_ref[...], *halo, ok)
    u = advance_many(p, vx, vy, vz, c2, DT, 4, ok[0], ok[2], loads)[-1]
    out[...] = u
    put_far((far_e, far_o), ways()[1], u)
    med[...] = c2
    at = 0
    for load in loads:
        at = put(loads_out, at, load)


def kept_loads(loads_ref, base=0):
    starts = [base + sum(LOADS[:i]) for i in range(4)]
    return [loads_ref[start : start + n] for start, n in zip(starts, LOADS)]


def residue_kernel(relaxed, loads_ref, med, e2, o2, e1, o1, own, out, back):
    ok = flags()
    p, vx, vy, vz = wide(own[...], *halo_of((e1, o1), (e2, o2)), ok)
    u = advance_many(p, vx, vy, vz, med[...], DT, 4, ok[0], ok[2], kept_loads(loads_ref))[-1]
    out[...] = u - relaxed[...]
    put(back, put(back, 0, u), loads_ref[...])


def gram_kernel(parts, basis, *refs):
    before = refs[0] if len(refs) == 3 else None
    out, split = refs[-2:]
    rows = 16

    def step(i, total):
        for j in range(rows):
            values = basis[pl.ds(i * rows + j, RANK, stride=8 * NX), :]
            high = values.astype(BF16)
            rest = values - high.astype(F32)
            middle = rest.astype(BF16)
            low = (rest - middle.astype(F32)).astype(BF16)
            lanes = slice(j * NY, (j + 1) * NY)
            split[0:RANK, lanes] = high
            split[RANK : 2 * RANK, lanes] = middle
            split[2 * RANK : 3 * RANK, lanes] = low
        both = split[...]
        return total + lax.dot_general(
            both, both, (((1,), (1,)), ((), ())), preferred_element_type=F32
        )

    total = lax.fori_loop(*parts, step, jnp.zeros((3 * RANK, 3 * RANK), F32))
    part = total[0:RANK] + total[RANK : 2 * RANK] + total[2 * RANK :]
    gram = part[:, 0:RANK] + part[:, RANK : 2 * RANK] + part[:, 2 * RANK :]
    gram = jnp.concatenate([gram, gram], axis=1)
    out[...] = gram if before is None else gram + before[...]


def inner_products(basis, u, scratch):
    tiles = u.reshape(8 * NX, NY)
    pieces = [tiles[8 * i : 8 * i + 8] for i in range(NX)]
    for r in range(RANK):
        at = r * 8 * NX
        sums = []
        for lane in range(4):
            part = basis[at + 32 * lane : at + 32 * lane + 8, :] * pieces[4 * lane]
            for i in range(1, 4):
                low = at + 32 * lane + 8 * i
                part = part + basis[low : low + 8, :] * pieces[4 * lane + i]
            sums.append(part)
        total = (sums[0] + sums[1]) + (sums[2] + sums[3])
        scratch[r : r + 1, :] = jnp.sum(total, axis=0, keepdims=True)
    column = jnp.sum(scratch[...], axis=1, keepdims=True)
    return to_row(column)


def to_row(column):
    r = lax.broadcasted_iota(jnp.int32, (RANK, NY), 0)
    lane = lax.broadcasted_iota(jnp.int32, (RANK, NY), 1)
    return jnp.sum(jnp.where(r == lane, column, 0.0), axis=0, keepdims=True)


def first_kernel(basis, x_ref, gram, out, scratch):
    row = inner_products(basis, x_ref[...], scratch)
    g = gram[...]
    lane = lax.broadcasted_iota(jnp.int32, (RANK // 2, NY), 1)
    packed = jnp.where(lane < RANK, g[: RANK // 2], g[RANK // 2 :])
    rows = jnp.concatenate([packed, jnp.broadcast_to(row, (8, NY))], axis=0)
    for j in range(N_SP):
        out[j] = rows


def inverse(g):
    lane = lax.broadcasted_iota(jnp.int32, (RANK, NY), 1)
    row = lax.broadcasted_iota(jnp.int32, (RANK, NY), 0)
    work = jnp.where(lane < RANK, g, jnp.where(lane - RANK == row, 1.0, 0.0))
    block = 8
    for start in range(0, RANK, block):
        columns = [
            jnp.broadcast_to(work[:, j : j + 1], (RANK, NY)) for j in range(start, start + block)
        ]
        for i in range(block):
            j = start + i
            reciprocal = 1.0 / columns[i][j : j + 1, :]
            factor = jnp.where(row == j, 0.0, columns[i])
            for later in range(i + 1, block):
                scaled = columns[later][j : j + 1, :] * reciprocal
                columns[later] = columns[later] - factor * scaled
            work = work - factor * (work[j : j + 1, :] * reciprocal)
    diagonal = jnp.sum(jnp.where(lane == row, work, 0.0), axis=1, keepdims=True)
    solved = pltpu.roll(work, RANK, 1) * (1.0 / diagonal)
    return jnp.where(lane < RANK, solved, 0.0)


def project(basis, ginv, coef, x, scratch, outs):
    weights = jnp.sum(ginv * coef, axis=1, keepdims=True)
    scratch[...] = jnp.broadcast_to(weights, (RANK, NY))
    total = [jnp.zeros((8, NY), F32) for _ in range(NX)]
    for r in range(RANK):
        w = scratch[r : r + 1, :]
        at = r * 8 * NX
        for i in range(NX):
            total[i] = total[i] + w * basis[at + 8 * i : at + 8 * i + 8, :]
    y = jnp.concatenate(total, axis=0).reshape(8, NX, NY)
    z = x - y
    center, e1, o1, e2, o2 = outs
    put(center, 0, y)
    put(center, 8, z)
    up1, up2 = ways()
    put_both((e1, o1), up1, 0, [y], [z[1:2], z[7:8]], [z[0:1], z[6:7]])
    put_far((e2, o2), up2, y)


PROJECTED = [(16, NX, NY), (10, NX, NY), (10, NX, NY), (6, NX, NY), (6, NX, NY)]


def first_project_kernel(got, basis, x_ref, ginv_ref, *rest):
    outs, scratch = rest[:5], rest[5]
    total = got[0]
    for j in range(1, N_SP):
        total = total + got[j]
    packed = total[: RANK // 2]
    g = jnp.concatenate([packed, pltpu.roll(packed, RANK, 1)], axis=0)
    ginv = inverse(g)
    ginv_ref[...] = ginv
    project(basis, ginv, total[RANK // 2 : RANK // 2 + 1], x_ref[...], scratch, outs)


def project_kernel(got, ginv_ref, basis, x_ref, *rest):
    outs, scratch = rest[:5], rest[5]
    coef = jnp.sum(got[...], axis=0)
    project(basis, ginv_ref[...], coef, x_ref[...], scratch, outs)


def q_of(med, e2, o2, e1, o1, center):
    ok = flags()
    c2 = med[...]
    y = center[0:8]
    z = center[8:16]
    halo = halo_of((e1, o1), (e2, o2))
    b1, a1 = halo[:2]
    p, vx, vy, vz = wide(y, *halo, ok)
    fine = advance_many(p, vx, vy, vz, c2, DT, 4, ok[0], ok[2])[-1]
    zp = cat(only(ok[0], b1[8:9]), z[0:2], only(ok[1], a1[8:9]))
    zz = cat(b1[9:10], z[6:8])
    coarse = advance_many(zp, z[2:4], z[4:6], zz, c2[3:5], 4 * DT, 1, ok[0], ok[2])[-1]
    return fine + coarse


def put_copies(ref, row):
    for j in range(N_SP):
        ref[j] = row


def level_kernel(med, e2, o2, e1, o1, center, acc, basis, u_out, acc_out, row_out, scratch):
    u = q_of(med, e2, o2, e1, o1, center)
    u_out[...] = u
    acc_out[...] = acc[...] + u
    put_copies(row_out, inner_products(basis, u, scratch))


def gap_kernel(med, e2, o2, e1, o1, center, acc, u_out, acc_out, e_out, o_out):
    u = q_of(med, e2, o2, e1, o1, center)
    u_out[...] = u
    acc_out[...] = acc[...] + u
    put_far((e_out, o_out), ways()[0], u)


def chain_kernel(med, o1, e1, own, acc, basis, x_out, row_out, scratch):
    ok = flags()
    b, a = below_above(ways()[0], e1, o1)
    p = cat(only(ok[0], b[0:2]), own[0:2], only(ok[1], a[0:2]))
    vx = cat(b[4:5], own[2:4], a[4:5])
    vy = cat(b[5:6], own[4:6], a[5:6])
    vz = cat(b[2:4], own[6:8], a[2:3])
    c2 = med[...]
    moved_on = advance_many(p, vx, vy, vz, c2[2:6], 8 * DT, 2, ok[0], ok[2])[-1]
    row = lax.axis_index("tm")
    chained = (row >= 5) | (row == 0)
    x = acc[...] + only(chained, moved_on)
    x_out[...] = x
    put_copies(row_out, inner_products(basis, x, scratch))


def final_kernel(med, e2, o2, e1, o1, center, back, basis, out, e_out, o_out, row_out, scratch):
    u = q_of(med, e2, o2, e1, o1, center) + back[0:8]
    out[...] = u
    up2 = ways()[1]
    put_both((e_out, o_out), up2, 0, [], [u[1:2], u[7:8]], [u[0:1], u[6:7]])
    put_copies(row_out, inner_products(basis, u, scratch))


def sweep_kernel(back, med, final, e2, o2, e1, o1, own, got, ginv, out, coords, kept, kept_row, sems):
    def copy(row, source):
        return pltpu.make_async_copy(source, out.at[row], sems.at[row])

    copies = [copy(3, final)]
    copies[0].start()
    coef = jnp.sum(got[...], axis=0)
    kept_row[...] = to_row(jnp.sum(ginv[...] * coef, axis=1, keepdims=True))
    copies.append(pltpu.make_async_copy(kept_row, coords, sems.at[4]))
    copies[1].start()
    ok = flags()
    loads = [load[1:-1] for load in kept_loads(back, 8)[:3]]
    b1, a1, b2, a2 = halo_of((e1, o1), (e2, o2))
    u = own[...]
    p = cat(
        only(ok[2], b2[0:1]), only(ok[0], b1[0:2]), u[0:2], only(ok[1], a1[0:2]), only(ok[3], a2[0:1])
    )
    vx = cat(b1[2:4], u[2:4], a1[2:4])
    vy = cat(b1[4:6], u[4:6], a1[4:6])
    vz = cat(b2[1:2], b1[6:8], u[6:8], a1[6:8])
    points = advance_many(p, vx, vy, vz, med[1:7], DT, 3, ok[0], ok[2], loads)
    for i in range(3):
        kept[i] = points[i]
        copies.append(copy(i, kept.at[i]))
        copies[-1].start()
    for each in copies:
        each.wait()


def body(speed, forcing, guess, basis):
    columns = basis.reshape(RANK * 8 * NX, NY)
    state = (8, NX, NY)
    table = [pltpu.VMEM((RANK, NY), F32)]
    split = [pltpu.VMEM((3 * RANK, 16 * NY), BF16)]
    copies = (N_SP, 1, NY)
    far = [(6, NX, NY), (6, NX, NY)]

    def traded(near, distant, center, by_tm):
        far_second = trade(distant[1], by_tm, 2, False)
        far_first = trade(distant[0], by_tm, 2, True)
        near_second = trade(near[1], by_tm, 1, False)
        near_first = trade(near[0], by_tm, 1, True)
        result = [far_first, far_second, near_first, near_second]
        if by_tm:
            result.append(hop(center, by_tm))
        return result

    start = hop(guess.reshape(state), 2)
    load = hop(forcing, 1)
    (c2,) = call(stage_kernel, [(2, NX, NY)], speed, columns)
    e1, o1, e2, o2 = call(
        pack_kernel, [(15, NX, NY), (15, NX, NY), (8, NX, NY), (8, NX, NY)], start, load, c2
    )
    e2, o2, e1, o1 = traded((e1, o1), (e2, o2), None, 0)
    (gram,) = call(
        functools.partial(gram_kernel, (0, 4)), [(RANK, NY)], columns, scratch=split, flops=50_000_000
    )
    relaxed, e, o, med, loads = call(
        relax_kernel,
        [state, *far, (8, NX, NY), (sum(LOADS), NX, NY)],
        start,
        load,
        c2,
        e1,
        o1,
        e2,
        o2,
    )
    near = traded((relaxed, relaxed), (e, o), relaxed, 1)
    (gram,) = call(functools.partial(gram_kernel, (4, 8)), [(RANK, NY)], columns, gram, scratch=split, flops=50_000_000)
    x, back = call(residue_kernel, [state, (8 + sum(LOADS), NX, NY)], relaxed, loads, med, *near)
    back = hop(back, -1)
    (rows,) = call(first_kernel, [(N_SP, RANK // 2 + 8, NY)], columns, x, gram, scratch=table)
    ginv, *packed = call(
        first_project_kernel, [(RANK, NY), *PROJECTED], share(rows), columns, x, scratch=table
    )

    def exchanged(packed, by_tm):
        center, e1, o1, e2, o2 = packed
        result = traded((e1, o1), (e2, o2), center, by_tm)
        return result if by_tm else result + [center]

    acc = x
    for _ in range(2):
        u, acc, rows = call(
            level_kernel, [state, state, copies], med, *exchanged(packed, 1), acc, columns, scratch=table
        )
        packed = call(project_kernel, PROJECTED, share(rows), ginv, columns, u, scratch=table)
    gap, acc, e, o = call(gap_kernel, [state, state, *far], med, *exchanged(packed, 1), acc)
    o = trade(o, 4, 1, False)
    e = trade(e, 4, 1, True)
    x, rows = call(
        chain_kernel, [state, copies], med, o, e, hop(gap, 4), acc, columns, scratch=table
    )
    packed = call(project_kernel, PROJECTED, share(rows), ginv, columns, x, scratch=table)
    final, e, o, rows = call(
        final_kernel,
        [state, (2, NX, NY), (2, NX, NY), copies],
        med,
        *exchanged(packed, 0),
        back,
        columns,
        scratch=table,
    )
    got = share(rows)
    near = traded((final, final), (e, o), final, 1)
    states, coords = call(
        sweep_kernel,
        [(4, 8, NX, NY), (1, NY)],
        back,
        med,
        final,
        *near,
        got,
        ginv,
        scratch=[pltpu.VMEM((3, 8, NX, NY), F32), pltpu.VMEM((1, NY), F32), pltpu.SemaphoreType.DMA((5,))],
        outward=True,
    )
    return states.reshape(4, 4, 2, NX, NY), coords[:, :RANK]


def solution(mesh):
    placed = (
        P("space", None, None),
        P("tm", "space", None, None),
        P("tm", None, "space", None, None),
        P("tm", None, None, "space", None, None),
    )
    return jax.shard_map(
        body,
        mesh=mesh,
        in_specs=placed,
        out_specs=(P("tm", None, "space", None, None), P("tm", None)),
        check_vma=False,
    )
```

```python
import functools

import jax
import jax.numpy as jnp
from jax import lax
from jax.experimental import pallas as pl
from jax.experimental.pallas import tpu as pltpu
from jax.sharding import PartitionSpec as P


DT = 0.045
N_TM = 8
N_SP = 16
RANK = 64
NX = 16
NY = 128
F32 = jnp.float32
BF16 = jnp.bfloat16
VMEM = pl.BlockSpec(memory_space=pltpu.VMEM)


def moved(value, by_tm, other):
    pairs = []
    for k in range(N_TM):
        for s in range(N_SP):
            slab = other(s)
            if 0 <= slab < N_SP:
                target = ((k + by_tm) % N_TM) * N_SP + slab
            else:
                target = ((k + (by_tm or 1)) % N_TM) * N_SP + s
            pairs.append((k * N_SP + s, target))
    return lax.ppermute(value, ("tm", "space"), pairs)


def hop(value, by_tm):
    return moved(value, by_tm, lambda s: s)


def trade(value, by_tm, step, first):
    low = 0 if first else 1

    def other(s):
        return s + step if (s // step) % 2 == low else s - step

    return moved(value, by_tm, other)


def share(copies):
    return lax.all_to_all(copies, "space", 0, 0, tiled=True)


def next_x(v):
    row = lax.broadcasted_iota(jnp.int32, v.shape, 1)
    return jnp.where(row < NX - 1, pltpu.roll(v, NX - 1, 1), 0.0)


def prev_x(v):
    row = lax.broadcasted_iota(jnp.int32, v.shape, 1)
    return jnp.where(row > 0, pltpu.roll(v, 1, 1), 0.0)


def next_y(v):
    lane = lax.broadcasted_iota(jnp.int32, v.shape, 2)
    return jnp.where(lane < NY - 1, pltpu.roll(v, NY - 1, 2), 0.0)


def prev_y(v):
    lane = lax.broadcasted_iota(jnp.int32, v.shape, 2)
    return jnp.where(lane > 0, pltpu.roll(v, 1, 2), 0.0)


def cat(*parts):
    parts = [part for part in parts if part.shape[0]]
    return parts[0] if len(parts) == 1 else jnp.concatenate(parts, axis=0)


def only(ok, v):
    return jnp.where(ok, v, jnp.zeros_like(v))


def without_floor(vz, low, ok1, ok2):
    far = max(0, low - 2)
    return cat(only(ok2, vz[:far]), only(ok1, vz[far:low]), vz[low:])


def advance_many(p, vx, vy, vz, c2, h, steps, ok1, ok2, loads=None):
    wx, wy = prev_x(vx), prev_y(vy)
    points = []
    for i in range(steps):
        low = steps - i
        mid = p[1:-1]
        row = lax.broadcasted_iota(jnp.int32, mid.shape, 1)
        lane = lax.broadcasted_iota(jnp.int32, mid.shape, 2)
        vx = vx - h * (next_x(mid) - mid)
        vy = vy - h * (next_y(mid) - mid)
        wx = jnp.where(row > 0, wx - h * (mid - pltpu.roll(mid, 1, 1)), 0.0)
        wy = jnp.where(lane > 0, wy - h * (mid - pltpu.roll(mid, 1, 2)), 0.0)
        vz = vz - h * (p[1:] - p[:-1])
        vz = without_floor(vz, low, ok1, ok2)
        diverge = (vx - wx) + (vy - wy) + (vz[1:] - vz[:-1])
        p = mid - h * c2 * diverge
        if loads is not None:
            p = p + loads[i]
        edge = low - 1
        n = p.shape[0]
        own = slice(edge, n - edge)
        points.append(cat(p[own], vx[own], vy[own], vz[1:][own]))
        vx, vy, wx, wy, c2 = (v[1:-1] for v in (vx, vy, wx, wy, c2))
        vz = vz[1:n]
    return points


def put(ref, at, planes):
    n = planes.shape[0]
    ref[at : at + n] = planes
    return at + n


def put_both(refs, up_first, at, both, up=(), down=()):
    first, second = refs
    for planes in both:
        put(first, at, planes)
        at = put(second, at, planes)
    for rising, falling in zip(up, down):
        put(first, at, jnp.where(up_first, rising, falling))
        at = put(second, at, jnp.where(up_first, falling, rising))
    return at


def put_far(refs, up_first, u, more_up=(), more_down=()):
    up = [u[3:4], u[5:6], *more_up]
    down = [u[2:3], u[4:5], *more_down]
    put_both(refs, up_first, 0, [u[0:2], u[6:8]], up, down)


def below_above(up_first, first, second):
    a, b = first[...], second[...]
    return jnp.where(up_first, b, a), jnp.where(up_first, a, b)


def wide(own, b1, a1, b2, a2, ok):
    ok_b1, ok_a1, ok_b2, ok_a2 = ok
    p = cat(
        only(ok_b2, b2[0:2]), only(ok_b1, b1[0:2]), own[0:2], only(ok_a1, a1[0:2]), only(ok_a2, a2[0:2])
    )
    vx = cat(b2[4:5], b1[2:4], own[2:4], a1[2:4], a2[4:5])
    vy = cat(b2[5:6], b1[4:6], own[4:6], a1[4:6], a2[5:6])
    vz = cat(b2[2:4], b1[6:8], own[6:8], a1[6:8], a2[2:3])
    return p, vx, vy, vz


def flags():
    s = lax.axis_index("space")
    return s >= 1, s < N_SP - 1, s >= 2, s < N_SP - 2


def ways():
    s = lax.axis_index("space")
    return (s & 1) == 0, (s & 2) == 0


def halo_of(near, far):
    up1, up2 = ways()
    return *below_above(up1, *near), *below_above(up2, *far)


def call(kernel, outs, *args, scratch=(), flops=1_000_000, limit=4, outward=False):
    kind = pltpu.HBM if outward else pltpu.VMEM
    shapes = [kind(shape, F32) for shape in outs]
    args = [pltpu.with_memory_space_constraint(arg, pltpu.VMEM) for arg in args]
    return pl.pallas_call(
        kernel,
        out_shape=shapes,
        in_specs=[VMEM] * len(args),
        out_specs=[pl.BlockSpec(memory_space=kind)] * len(shapes),
        scratch_shapes=list(scratch),
        compiler_params=pltpu.CompilerParams(vmem_limit_bytes=limit * 1024 * 1024),
        cost_estimate=pl.CostEstimate(flops=flops, bytes_accessed=100_000, transcendentals=0),
    )(*args)


def stage_kernel(c_ref, basis, c2_out):
    c2_out[...] = c_ref[...] * c_ref[...]


def pack_kernel(g_ref, f_ref, c2_ref, e1, o1, e2, o2):
    up1, up2 = ways()
    u = g_ref[...]
    c2 = c2_ref[...]
    put_both((e1, o1), up1, 0, [u, f_ref[0], f_ref[1], c2], [f_ref[2, 1:2]], [f_ref[2, 0:1]])
    put_far((e2, o2), up2, u, [f_ref[0, 1:2], c2[1:2]], [f_ref[0, 0:1], c2[0:1]])


def load_medium(own, b1, a1, b2, a2, ok):
    ok_b1, ok_a1, ok_b2, ok_a2 = ok
    return cat(
        only(ok_b2, b2[7:8]), only(ok_b1, b1[12:14]), own, only(ok_a1, a1[12:14]), only(ok_a2, a2[7:8])
    )


def load_forcing(f_ref, b1, a1, b2, a2, ok):
    ok_b1, ok_a1, ok_b2, ok_a2 = ok
    return [
        cat(
            only(ok_b2, b2[6:7]), only(ok_b1, b1[8:10]), f_ref[0], only(ok_a1, a1[8:10]), only(ok_a2, a2[6:7])
        ),
        cat(only(ok_b1, b1[10:12]), f_ref[1], only(ok_a1, a1[10:12])),
        cat(only(ok_b1, b1[14:15]), f_ref[2], only(ok_a1, a1[14:15])),
        f_ref[3],
    ]


LOADS = [8, 6, 4, 2]


def relax_kernel(g_ref, f_ref, c2_ref, e1, o1, e2, o2, out, far_e, far_o, med, loads_out):
    ok = flags()
    halo = halo_of((e1, o1), (e2, o2))
    c2 = load_medium(c2_ref[...], *halo, ok)
    loads = load_forcing(f_ref, *halo, ok)
    p, vx, vy, vz = wide(g_ref[...], *halo, ok)
    u = advance_many(p, vx, vy, vz, c2, DT, 4, ok[0], ok[2], loads)[-1]
    out[...] = u
    put_far((far_e, far_o), ways()[1], u)
    med[...] = c2
    at = 0
    for load in loads:
        at = put(loads_out, at, load)


def kept_loads(loads_ref):
    starts = [sum(LOADS[:i]) for i in range(4)]
    return [loads_ref[start : start + n] for start, n in zip(starts, LOADS)]


def residue_kernel(relaxed, loads_ref, med, e2, o2, e1, o1, own, out, back):
    ok = flags()
    p, vx, vy, vz = wide(own[...], *halo_of((e1, o1), (e2, o2)), ok)
    u = advance_many(p, vx, vy, vz, med[...], DT, 4, ok[0], ok[2], kept_loads(loads_ref))[-1]
    out[...] = u - relaxed[...]
    at = put(back, 0, u)
    for load in kept_loads(loads_ref)[:3]:
        at = put(back, at, load[1:-1])


def gram_kernel(parts, basis, *refs):
    before = refs[0] if len(refs) == 3 else None
    out, split = refs[-2:]
    rows = 16

    def step(i, total):
        for j in range(rows):
            values = basis[pl.ds(i * rows + j, RANK, stride=8 * NX), :]
            high = values.astype(BF16)
            rest = values - high.astype(F32)
            middle = rest.astype(BF16)
            low = (rest - middle.astype(F32)).astype(BF16)
            lanes = slice(j * NY, (j + 1) * NY)
            split[0:RANK, lanes] = high
            split[RANK : 2 * RANK, lanes] = middle
            split[2 * RANK : 3 * RANK, lanes] = low
        both = split[...]
        return total + lax.dot_general(
            both, both, (((1,), (1,)), ((), ())), preferred_element_type=F32
        )

    total = lax.fori_loop(*parts, step, jnp.zeros((3 * RANK, 3 * RANK), F32))
    part = total[0:RANK] + total[RANK : 2 * RANK] + total[2 * RANK :]
    gram = part[:, 0:RANK] + part[:, RANK : 2 * RANK] + part[:, 2 * RANK :]
    gram = jnp.concatenate([gram, gram], axis=1)
    out[...] = gram if before is None else gram + before[...]


def inner_products(basis, u, scratch):
    tiles = u.reshape(8 * NX, NY)
    pieces = [tiles[8 * i : 8 * i + 8] for i in range(NX)]
    for r in range(RANK):
        at = r * 8 * NX
        sums = []
        for lane in range(4):
            part = basis[at + 32 * lane : at + 32 * lane + 8, :] * pieces[4 * lane]
            for i in range(1, 4):
                low = at + 32 * lane + 8 * i
                part = part + basis[low : low + 8, :] * pieces[4 * lane + i]
            sums.append(part)
        total = (sums[0] + sums[1]) + (sums[2] + sums[3])
        scratch[r : r + 1, :] = jnp.sum(total, axis=0, keepdims=True)
    column = jnp.sum(scratch[...], axis=1, keepdims=True)
    return to_row(column)


def to_row(column):
    r = lax.broadcasted_iota(jnp.int32, (RANK, NY), 0)
    lane = lax.broadcasted_iota(jnp.int32, (RANK, NY), 1)
    return jnp.sum(jnp.where(r == lane, column, 0.0), axis=0, keepdims=True)


def first_kernel(basis, x_ref, gram, out, scratch):
    row = inner_products(basis, x_ref[...], scratch)
    g = gram[...]
    lane = lax.broadcasted_iota(jnp.int32, (RANK // 2, NY), 1)
    packed = jnp.where(lane < RANK, g[: RANK // 2], g[RANK // 2 :])
    rows = jnp.concatenate([packed, jnp.broadcast_to(row, (8, NY))], axis=0)
    for j in range(N_SP):
        out[j] = rows


def inverse(g):
    lane = lax.broadcasted_iota(jnp.int32, (RANK, NY), 1)
    row = lax.broadcasted_iota(jnp.int32, (RANK, NY), 0)
    work = jnp.where(lane < RANK, g, jnp.where(lane - RANK == row, 1.0, 0.0))
    block = 8
    for start in range(0, RANK, block):
        columns = [
            jnp.broadcast_to(work[:, j : j + 1], (RANK, NY)) for j in range(start, start + block)
        ]
        for i in range(block):
            j = start + i
            reciprocal = 1.0 / columns[i][j : j + 1, :]
            factor = jnp.where(row == j, 0.0, columns[i])
            for later in range(i + 1, block):
                scaled = columns[later][j : j + 1, :] * reciprocal
                columns[later] = columns[later] - factor * scaled
            work = work - factor * (work[j : j + 1, :] * reciprocal)
    diagonal = jnp.sum(jnp.where(lane == row, work, 0.0), axis=1, keepdims=True)
    solved = pltpu.roll(work, RANK, 1) * (1.0 / diagonal)
    return jnp.where(lane < RANK, solved, 0.0)


def project(basis, ginv, coef, x, scratch, outs):
    weights = jnp.sum(ginv * coef, axis=1, keepdims=True)
    scratch[...] = jnp.broadcast_to(weights, (RANK, NY))
    total = [jnp.zeros((8, NY), F32) for _ in range(NX)]
    for r in range(RANK):
        w = scratch[r : r + 1, :]
        at = r * 8 * NX
        for i in range(NX):
            total[i] = total[i] + w * basis[at + 8 * i : at + 8 * i + 8, :]
    y = jnp.concatenate(total, axis=0).reshape(8, NX, NY)
    z = x - y
    center, e1, o1, e2, o2 = outs
    put(center, 0, y)
    put(center, 8, z)
    up1, up2 = ways()
    put_both((e1, o1), up1, 0, [y], [z[1:2], z[7:8]], [z[0:1], z[6:7]])
    put_far((e2, o2), up2, y)


PROJECTED = [(16, NX, NY), (10, NX, NY), (10, NX, NY), (6, NX, NY), (6, NX, NY)]


def first_project_kernel(got, basis, x_ref, ginv_ref, *rest):
    outs, scratch = rest[:5], rest[5]
    total = got[0]
    for j in range(1, N_SP):
        total = total + got[j]
    packed = total[: RANK // 2]
    g = jnp.concatenate([packed, pltpu.roll(packed, RANK, 1)], axis=0)
    ginv = inverse(g)
    ginv_ref[...] = ginv
    project(basis, ginv, total[RANK // 2 : RANK // 2 + 1], x_ref[...], scratch, outs)


def project_kernel(got, ginv_ref, basis, x_ref, *rest):
    outs, scratch = rest[:5], rest[5]
    coef = jnp.sum(got[...], axis=0)
    project(basis, ginv_ref[...], coef, x_ref[...], scratch, outs)


def q_of(med, e2, o2, e1, o1, center):
    ok = flags()
    c2 = med[...]
    y = center[0:8]
    z = center[8:16]
    halo = halo_of((e1, o1), (e2, o2))
    b1, a1 = halo[:2]
    p, vx, vy, vz = wide(y, *halo, ok)
    fine = advance_many(p, vx, vy, vz, c2, DT, 4, ok[0], ok[2])[-1]
    zp = cat(only(ok[0], b1[8:9]), z[0:2], only(ok[1], a1[8:9]))
    zz = cat(b1[9:10], z[6:8])
    coarse = advance_many(zp, z[2:4], z[4:6], zz, c2[3:5], 4 * DT, 1, ok[0], ok[2])[-1]
    return fine + coarse


def put_copies(ref, row):
    for j in range(N_SP):
        ref[j] = row


def level_kernel(med, e2, o2, e1, o1, center, acc, basis, u_out, acc_out, row_out, scratch):
    u = q_of(med, e2, o2, e1, o1, center)
    u_out[...] = u
    acc_out[...] = acc[...] + u
    put_copies(row_out, inner_products(basis, u, scratch))


def gap_kernel(med, e2, o2, e1, o1, center, acc, u_out, acc_out, e_out, o_out):
    u = q_of(med, e2, o2, e1, o1, center)
    u_out[...] = u
    acc_out[...] = acc[...] + u
    put_far((e_out, o_out), ways()[0], u)


def chain_kernel(med, o1, e1, own, acc, basis, x_out, row_out, scratch):
    ok = flags()
    b, a = below_above(ways()[0], e1, o1)
    p = cat(only(ok[0], b[0:2]), own[0:2], only(ok[1], a[0:2]))
    vx = cat(b[4:5], own[2:4], a[4:5])
    vy = cat(b[5:6], own[4:6], a[5:6])
    vz = cat(b[2:4], own[6:8], a[2:3])
    c2 = med[...]
    moved_on = advance_many(p, vx, vy, vz, c2[2:6], 8 * DT, 2, ok[0], ok[2])[-1]
    row = lax.axis_index("tm")
    chained = (row >= 5) | (row == 0)
    x = acc[...] + only(chained, moved_on)
    x_out[...] = x
    put_copies(row_out, inner_products(basis, x, scratch))


def final_kernel(med, e2, o2, e1, o1, center, back, basis, out, e_out, o_out, row_out, scratch):
    u = q_of(med, e2, o2, e1, o1, center) + back[0:8]
    out[...] = u
    up2 = ways()[1]
    put_both((e_out, o_out), up2, 0, [], [u[1:2], u[7:8]], [u[0:1], u[6:7]])
    put_copies(row_out, inner_products(basis, u, scratch))


def sweep_kernel(back, med, final, e2, o2, e1, o1, own, got, ginv, out, coords, kept, kept_row, sems):
    def copy(row, source):
        return pltpu.make_async_copy(source, out.at[row], sems.at[row])

    copies = [copy(3, final)]
    copies[0].start()
    coef = jnp.sum(got[...], axis=0)
    kept_row[...] = to_row(jnp.sum(ginv[...] * coef, axis=1, keepdims=True))
    copies.append(pltpu.make_async_copy(kept_row, coords, sems.at[4]))
    copies[1].start()
    ok = flags()
    loads = [back[8:14], back[14:18], back[18:20]]
    b1, a1, b2, a2 = halo_of((e1, o1), (e2, o2))
    u = own[...]
    p = cat(
        only(ok[2], b2[0:1]), only(ok[0], b1[0:2]), u[0:2], only(ok[1], a1[0:2]), only(ok[3], a2[0:1])
    )
    vx = cat(b1[2:4], u[2:4], a1[2:4])
    vy = cat(b1[4:6], u[4:6], a1[4:6])
    vz = cat(b2[1:2], b1[6:8], u[6:8], a1[6:8])
    points = advance_many(p, vx, vy, vz, med[1:7], DT, 3, ok[0], ok[2], loads)
    for i in range(3):
        kept[i] = points[i]
        copies.append(copy(i, kept.at[i]))
        copies[-1].start()
    for each in copies:
        each.wait()


def body(speed, forcing, guess, basis):
    columns = basis.reshape(RANK * 8 * NX, NY)
    state = (8, NX, NY)
    table = [pltpu.VMEM((RANK, NY), F32)]
    split = [pltpu.VMEM((3 * RANK, 16 * NY), BF16)]
    copies = (N_SP, 1, NY)
    far = [(6, NX, NY), (6, NX, NY)]

    def traded(near, distant, center, by_tm):
        far_second = trade(distant[1], by_tm, 2, False)
        far_first = trade(distant[0], by_tm, 2, True)
        near_second = trade(near[1], by_tm, 1, False)
        near_first = trade(near[0], by_tm, 1, True)
        result = [far_first, far_second, near_first, near_second]
        if by_tm:
            result.append(hop(center, by_tm))
        return result

    start = hop(guess.reshape(state), 2)
    load = hop(forcing, 1)
    (c2,) = call(stage_kernel, [(2, NX, NY)], speed, columns)
    e1, o1, e2, o2 = call(
        pack_kernel, [(15, NX, NY), (15, NX, NY), (8, NX, NY), (8, NX, NY)], start, load, c2
    )
    e2, o2, e1, o1 = traded((e1, o1), (e2, o2), None, 0)
    (gram,) = call(
        functools.partial(gram_kernel, (0, 4)), [(RANK, NY)], columns, scratch=split, flops=50_000_000
    )
    relaxed, e, o, med, loads = call(
        relax_kernel,
        [state, *far, (8, NX, NY), (sum(LOADS), NX, NY)],
        start,
        load,
        c2,
        e1,
        o1,
        e2,
        o2,
    )
    near = traded((relaxed, relaxed), (e, o), relaxed, 1)
    (gram,) = call(
        functools.partial(gram_kernel, (4, 8)), [(RANK, NY)], columns, gram, scratch=split, flops=50_000_000
    )
    x, back = call(residue_kernel, [state, (20, NX, NY)], relaxed, loads, med, *near)
    back = hop(back, -1)
    (rows,) = call(first_kernel, [(N_SP, RANK // 2 + 8, NY)], columns, x, gram, scratch=table)
    ginv, *packed = call(
        first_project_kernel, [(RANK, NY), *PROJECTED], share(rows), columns, x, scratch=table
    )

    def exchanged(packed, by_tm):
        center, e1, o1, e2, o2 = packed
        result = traded((e1, o1), (e2, o2), center, by_tm)
        return result if by_tm else result + [center]

    acc = x
    for _ in range(2):
        u, acc, rows = call(
            level_kernel, [state, state, copies], med, *exchanged(packed, 1), acc, columns, scratch=table
        )
        packed = call(project_kernel, PROJECTED, share(rows), ginv, columns, u, scratch=table)
    gap, acc, e, o = call(gap_kernel, [state, state, *far], med, *exchanged(packed, 1), acc)
    e = trade(e, 4, 1, True)
    o = trade(o, 4, 1, False)
    gap = hop(gap, 4)
    x, rows = call(
        chain_kernel, [state, copies], med, o, e, gap, acc, columns, scratch=table
    )
    packed = call(project_kernel, PROJECTED, share(rows), ginv, columns, x, scratch=table)
    final, e, o, rows = call(
        final_kernel,
        [state, (2, NX, NY), (2, NX, NY), copies],
        med,
        *exchanged(packed, 0),
        back,
        columns,
        scratch=table,
    )
    got = share(rows)
    near = traded((final, final), (e, o), final, 1)
    states, coords = call(
        sweep_kernel,
        [(4, 8, NX, NY), (1, NY)],
        back,
        med,
        final,
        *near,
        got,
        ginv,
        scratch=[pltpu.VMEM((3, 8, NX, NY), F32), pltpu.VMEM((1, NY), F32), pltpu.SemaphoreType.DMA((5,))],
        outward=True,
    )
    return states.reshape(4, 4, 2, NX, NY), coords[:, :RANK]


def solution(mesh):
    placed = (
        P("space", None, None),
        P("tm", "space", None, None),
        P("tm", None, "space", None, None),
        P("tm", None, None, "space", None, None),
    )
    return jax.shard_map(
        body,
        mesh=mesh,
        in_specs=placed,
        out_specs=(P("tm", None, "space", None, None), P("tm", None)),
        check_vma=False,
    )
```

```python
import functools

import jax
import jax.numpy as jnp
from jax import lax
from jax.experimental import pallas as pl
from jax.experimental.pallas import tpu as pltpu
from jax.sharding import PartitionSpec as P


DT = 0.045
N_TM = 8
N_SP = 16
RANK = 64
NX = 16
NY = 128
F32 = jnp.float32
BF16 = jnp.bfloat16
VMEM = pl.BlockSpec(memory_space=pltpu.VMEM)


def moved(value, by_tm, other):
    pairs = []
    for k in range(N_TM):
        for s in range(N_SP):
            slab = other(s)
            if 0 <= slab < N_SP:
                target = ((k + by_tm) % N_TM) * N_SP + slab
            else:
                target = ((k + (by_tm or 1)) % N_TM) * N_SP + s
            pairs.append((k * N_SP + s, target))
    return lax.ppermute(value, ("tm", "space"), pairs)


def hop(value, by_tm):
    return moved(value, by_tm, lambda s: s)


def trade(value, by_tm, step, first):
    low = 0 if first else 1

    def other(s):
        return s + step if (s // step) % 2 == low else s - step

    return moved(value, by_tm, other)


def share(copies):
    return lax.all_to_all(copies, "space", 0, 0, tiled=True)


def next_x(v):
    row = lax.broadcasted_iota(jnp.int32, v.shape, 1)
    return jnp.where(row < NX - 1, pltpu.roll(v, NX - 1, 1), 0.0)


def prev_x(v):
    row = lax.broadcasted_iota(jnp.int32, v.shape, 1)
    return jnp.where(row > 0, pltpu.roll(v, 1, 1), 0.0)


def next_y(v):
    lane = lax.broadcasted_iota(jnp.int32, v.shape, 2)
    return jnp.where(lane < NY - 1, pltpu.roll(v, NY - 1, 2), 0.0)


def prev_y(v):
    lane = lax.broadcasted_iota(jnp.int32, v.shape, 2)
    return jnp.where(lane > 0, pltpu.roll(v, 1, 2), 0.0)


def cat(*parts):
    parts = [part for part in parts if part.shape[0]]
    return parts[0] if len(parts) == 1 else jnp.concatenate(parts, axis=0)


def only(ok, v):
    return jnp.where(ok, v, jnp.zeros_like(v))


def without_floor(vz, low, ok1, ok2):
    far = max(0, low - 2)
    return cat(only(ok2, vz[:far]), only(ok1, vz[far:low]), vz[low:])


def advance_many(p, vx, vy, vz, c2, h, steps, ok1, ok2, loads=None):
    wx, wy = prev_x(vx), prev_y(vy)
    points = []
    for i in range(steps):
        low = steps - i
        mid = p[1:-1]
        row = lax.broadcasted_iota(jnp.int32, mid.shape, 1)
        lane = lax.broadcasted_iota(jnp.int32, mid.shape, 2)
        vx = vx - h * (next_x(mid) - mid)
        vy = vy - h * (next_y(mid) - mid)
        wx = jnp.where(row > 0, wx - h * (mid - pltpu.roll(mid, 1, 1)), 0.0)
        wy = jnp.where(lane > 0, wy - h * (mid - pltpu.roll(mid, 1, 2)), 0.0)
        vz = vz - h * (p[1:] - p[:-1])
        vz = without_floor(vz, low, ok1, ok2)
        diverge = (vx - wx) + (vy - wy) + (vz[1:] - vz[:-1])
        p = mid - h * c2 * diverge
        if loads is not None:
            p = p + loads[i]
        edge = low - 1
        n = p.shape[0]
        own = slice(edge, n - edge)
        points.append(cat(p[own], vx[own], vy[own], vz[1:][own]))
        vx, vy, wx, wy, c2 = (v[1:-1] for v in (vx, vy, wx, wy, c2))
        vz = vz[1:n]
    return points


def put(ref, at, planes):
    n = planes.shape[0]
    ref[at : at + n] = planes
    return at + n


def put_both(refs, up_first, at, both, up=(), down=()):
    first, second = refs
    for planes in both:
        put(first, at, planes)
        at = put(second, at, planes)
    for rising, falling in zip(up, down):
        put(first, at, jnp.where(up_first, rising, falling))
        at = put(second, at, jnp.where(up_first, falling, rising))
    return at


def put_far(refs, up_first, u, more_up=(), more_down=()):
    up = [u[3:4], u[5:6], *more_up]
    down = [u[2:3], u[4:5], *more_down]
    put_both(refs, up_first, 0, [u[0:2], u[6:8]], up, down)


def below_above(up_first, first, second):
    a, b = first[...], second[...]
    return jnp.where(up_first, b, a), jnp.where(up_first, a, b)


def wide(own, b1, a1, b2, a2, ok):
    ok_b1, ok_a1, ok_b2, ok_a2 = ok
    p = cat(
        only(ok_b2, b2[0:2]), only(ok_b1, b1[0:2]), own[0:2], only(ok_a1, a1[0:2]), only(ok_a2, a2[0:2])
    )
    vx = cat(b2[4:5], b1[2:4], own[2:4], a1[2:4], a2[4:5])
    vy = cat(b2[5:6], b1[4:6], own[4:6], a1[4:6], a2[5:6])
    vz = cat(b2[2:4], b1[6:8], own[6:8], a1[6:8], a2[2:3])
    return p, vx, vy, vz


def flags():
    s = lax.axis_index("space")
    return s >= 1, s < N_SP - 1, s >= 2, s < N_SP - 2


def ways():
    s = lax.axis_index("space")
    return (s & 1) == 0, (s & 2) == 0


def halo_of(near, far):
    up1, up2 = ways()
    return *below_above(up1, *near), *below_above(up2, *far)


def call(kernel, outs, *args, scratch=(), flops=1_000_000, limit=4, outward=False):
    kind = pltpu.HBM if outward else pltpu.VMEM
    shapes = [kind(shape, F32) for shape in outs]
    args = [pltpu.with_memory_space_constraint(arg, pltpu.VMEM) for arg in args]
    return pl.pallas_call(
        kernel,
        out_shape=shapes,
        in_specs=[VMEM] * len(args),
        out_specs=[pl.BlockSpec(memory_space=kind)] * len(shapes),
        scratch_shapes=list(scratch),
        compiler_params=pltpu.CompilerParams(vmem_limit_bytes=limit * 1024 * 1024),
        cost_estimate=pl.CostEstimate(flops=flops, bytes_accessed=100_000, transcendentals=0),
    )(*args)


def stage_kernel(c_ref, basis, c2_out):
    c2_out[...] = c_ref[...] * c_ref[...]


def pack_kernel(g_ref, f_ref, c2_ref, e1, o1, e2, o2):
    up1, up2 = ways()
    u = g_ref[...]
    c2 = c2_ref[...]
    put_both((e1, o1), up1, 0, [u, f_ref[0], f_ref[1], c2], [f_ref[2, 1:2]], [f_ref[2, 0:1]])
    put_far((e2, o2), up2, u, [f_ref[0, 1:2], c2[1:2]], [f_ref[0, 0:1], c2[0:1]])


def load_medium(own, b1, a1, b2, a2, ok):
    ok_b1, ok_a1, ok_b2, ok_a2 = ok
    return cat(
        only(ok_b2, b2[7:8]), only(ok_b1, b1[12:14]), own, only(ok_a1, a1[12:14]), only(ok_a2, a2[7:8])
    )


def load_forcing(f_ref, b1, a1, b2, a2, ok):
    ok_b1, ok_a1, ok_b2, ok_a2 = ok
    return [
        cat(
            only(ok_b2, b2[6:7]), only(ok_b1, b1[8:10]), f_ref[0], only(ok_a1, a1[8:10]), only(ok_a2, a2[6:7])
        ),
        cat(only(ok_b1, b1[10:12]), f_ref[1], only(ok_a1, a1[10:12])),
        cat(only(ok_b1, b1[14:15]), f_ref[2], only(ok_a1, a1[14:15])),
        f_ref[3],
    ]


LOADS = [8, 6, 4, 2]


def relax_kernel(g_ref, f_ref, c2_ref, e1, o1, e2, o2, out, far_e, far_o, med, loads_out):
    ok = flags()
    halo = halo_of((e1, o1), (e2, o2))
    c2 = load_medium(c2_ref[...], *halo, ok)
    loads = load_forcing(f_ref, *halo, ok)
    p, vx, vy, vz = wide(g_ref[...], *halo, ok)
    u = advance_many(p, vx, vy, vz, c2, DT, 4, ok[0], ok[2], loads)[-1]
    out[...] = u
    put_far((far_e, far_o), ways()[1], u)
    med[...] = c2
    at = 0
    for load in loads:
        at = put(loads_out, at, load)


def kept_loads(loads_ref):
    starts = [sum(LOADS[:i]) for i in range(4)]
    return [loads_ref[start : start + n] for start, n in zip(starts, LOADS)]


def residue_kernel(relaxed, loads_ref, med, e2, o2, e1, o1, own, out, back):
    ok = flags()
    p, vx, vy, vz = wide(own[...], *halo_of((e1, o1), (e2, o2)), ok)
    u = advance_many(p, vx, vy, vz, med[...], DT, 4, ok[0], ok[2], kept_loads(loads_ref))[-1]
    out[...] = u - relaxed[...]
    at = put(back, 0, u)
    for load in kept_loads(loads_ref)[:3]:
        at = put(back, at, load[1:-1])


def gram_kernel(parts, basis, *refs):
    before = refs[0] if len(refs) == 3 else None
    out, split = refs[-2:]
    rows = 16

    def step(i, total):
        for j in range(rows):
            values = basis[pl.ds(i * rows + j, RANK, stride=8 * NX), :]
            high = values.astype(BF16)
            rest = values - high.astype(F32)
            middle = rest.astype(BF16)
            low = (rest - middle.astype(F32)).astype(BF16)
            lanes = slice(j * NY, (j + 1) * NY)
            split[0:RANK, lanes] = high
            split[RANK : 2 * RANK, lanes] = middle
            split[2 * RANK : 3 * RANK, lanes] = low
        both = split[...]
        return total + lax.dot_general(
            both, both, (((1,), (1,)), ((), ())), preferred_element_type=F32
        )

    total = lax.fori_loop(*parts, step, jnp.zeros((3 * RANK, 3 * RANK), F32))
    part = total[0:RANK] + total[RANK : 2 * RANK] + total[2 * RANK :]
    gram = part[:, 0:RANK] + part[:, RANK : 2 * RANK] + part[:, 2 * RANK :]
    gram = jnp.concatenate([gram, gram], axis=1)
    out[...] = gram if before is None else gram + before[...]


def inner_products(basis, u, scratch):
    tiles = u.reshape(8 * NX, NY)
    pieces = [tiles[8 * i : 8 * i + 8] for i in range(NX)]
    for r in range(RANK):
        at = r * 8 * NX
        sums = []
        for lane in range(4):
            part = basis[at + 32 * lane : at + 32 * lane + 8, :] * pieces[4 * lane]
            for i in range(1, 4):
                low = at + 32 * lane + 8 * i
                part = part + basis[low : low + 8, :] * pieces[4 * lane + i]
            sums.append(part)
        total = (sums[0] + sums[1]) + (sums[2] + sums[3])
        scratch[r : r + 1, :] = jnp.sum(total, axis=0, keepdims=True)
    column = jnp.sum(scratch[...], axis=1, keepdims=True)
    return to_row(column)


def to_row(column):
    r = lax.broadcasted_iota(jnp.int32, (RANK, NY), 0)
    lane = lax.broadcasted_iota(jnp.int32, (RANK, NY), 1)
    return jnp.sum(jnp.where(r == lane, column, 0.0), axis=0, keepdims=True)


def first_kernel(basis, x_ref, gram, out, scratch):
    row = inner_products(basis, x_ref[...], scratch)
    g = gram[...]
    lane = lax.broadcasted_iota(jnp.int32, (RANK // 2, NY), 1)
    packed = jnp.where(lane < RANK, g[: RANK // 2], g[RANK // 2 :])
    rows = jnp.concatenate([packed, jnp.broadcast_to(row, (8, NY))], axis=0)
    for j in range(N_SP):
        out[j] = rows


def inverse(g):
    lane = lax.broadcasted_iota(jnp.int32, (RANK, NY), 1)
    row = lax.broadcasted_iota(jnp.int32, (RANK, NY), 0)
    work = jnp.where(lane < RANK, g, jnp.where(lane - RANK == row, 1.0, 0.0))
    block = 8
    for start in range(0, RANK, block):
        columns = [
            jnp.broadcast_to(work[:, j : j + 1], (RANK, NY)) for j in range(start, start + block)
        ]
        for i in range(block):
            j = start + i
            reciprocal = 1.0 / columns[i][j : j + 1, :]
            factor = jnp.where(row == j, 0.0, columns[i])
            for later in range(i + 1, block):
                scaled = columns[later][j : j + 1, :] * reciprocal
                columns[later] = columns[later] - factor * scaled
            work = work - factor * (work[j : j + 1, :] * reciprocal)
    diagonal = jnp.sum(jnp.where(lane == row, work, 0.0), axis=1, keepdims=True)
    solved = pltpu.roll(work, RANK, 1) * (1.0 / diagonal)
    return jnp.where(lane < RANK, solved, 0.0)


def project(basis, ginv, coef, x, scratch, outs):
    weights = jnp.sum(ginv * coef, axis=1, keepdims=True)
    scratch[...] = jnp.broadcast_to(weights, (RANK, NY))
    total = [jnp.zeros((8, NY), F32) for _ in range(NX)]
    for r in range(RANK):
        w = scratch[r : r + 1, :]
        at = r * 8 * NX
        for i in range(NX):
            total[i] = total[i] + w * basis[at + 8 * i : at + 8 * i + 8, :]
    y = jnp.concatenate(total, axis=0).reshape(8, NX, NY)
    z = x - y
    center, e1, o1, e2, o2 = outs
    put(center, 0, y)
    put(center, 8, z)
    up1, up2 = ways()
    put_both((e1, o1), up1, 0, [y], [z[1:2], z[7:8]], [z[0:1], z[6:7]])
    put_far((e2, o2), up2, y)


PROJECTED = [(16, NX, NY), (10, NX, NY), (10, NX, NY), (6, NX, NY), (6, NX, NY)]


def first_project_kernel(got, basis, x_ref, ginv_ref, *rest):
    outs, scratch = rest[:5], rest[5]
    total = got[0]
    for j in range(1, N_SP):
        total = total + got[j]
    packed = total[: RANK // 2]
    g = jnp.concatenate([packed, pltpu.roll(packed, RANK, 1)], axis=0)
    ginv = inverse(g)
    ginv_ref[...] = ginv
    project(basis, ginv, total[RANK // 2 : RANK // 2 + 1], x_ref[...], scratch, outs)


def project_kernel(got, ginv_ref, basis, x_ref, *rest):
    outs, scratch = rest[:5], rest[5]
    coef = jnp.sum(got[...], axis=0)
    project(basis, ginv_ref[...], coef, x_ref[...], scratch, outs)


def q_of(med, e2, o2, e1, o1, center):
    ok = flags()
    c2 = med[...]
    y = center[0:8]
    z = center[8:16]
    halo = halo_of((e1, o1), (e2, o2))
    b1, a1 = halo[:2]
    p, vx, vy, vz = wide(y, *halo, ok)
    fine = advance_many(p, vx, vy, vz, c2, DT, 4, ok[0], ok[2])[-1]
    zp = cat(only(ok[0], b1[8:9]), z[0:2], only(ok[1], a1[8:9]))
    zz = cat(b1[9:10], z[6:8])
    coarse = advance_many(zp, z[2:4], z[4:6], zz, c2[3:5], 4 * DT, 1, ok[0], ok[2])[-1]
    return fine + coarse


def put_copies(ref, row):
    for j in range(N_SP):
        ref[j] = row


def level_kernel(med, e2, o2, e1, o1, center, acc, basis, u_out, acc_out, row_out, scratch):
    u = q_of(med, e2, o2, e1, o1, center)
    u_out[...] = u
    acc_out[...] = acc[...] + u
    put_copies(row_out, inner_products(basis, u, scratch))


def gap_kernel(med, e2, o2, e1, o1, center, acc, u_out, acc_out, e_out, o_out):
    u = q_of(med, e2, o2, e1, o1, center)
    u_out[...] = u
    acc_out[...] = acc[...] + u
    put_far((e_out, o_out), ways()[0], u)


def chain_kernel(med, o1, e1, own, acc, basis, x_out, row_out, scratch):
    ok = flags()
    b, a = below_above(ways()[0], e1, o1)
    p = cat(only(ok[0], b[0:2]), own[0:2], only(ok[1], a[0:2]))
    vx = cat(b[4:5], own[2:4], a[4:5])
    vy = cat(b[5:6], own[4:6], a[5:6])
    vz = cat(b[2:4], own[6:8], a[2:3])
    c2 = med[...]
    moved_on = advance_many(p, vx, vy, vz, c2[2:6], 8 * DT, 2, ok[0], ok[2])[-1]
    row = lax.axis_index("tm")
    chained = (row >= 5) | (row == 0)
    x = acc[...] + only(chained, moved_on)
    x_out[...] = x
    put_copies(row_out, inner_products(basis, x, scratch))


def products_kernel(basis, u_ref, row_out, scratch):
    put_copies(row_out, inner_products(basis, u_ref[...], scratch))


def final_kernel(med, e2, o2, e1, o1, center, back, out, e_out, o_out):
    u = q_of(med, e2, o2, e1, o1, center) + back[0:8]
    out[...] = u
    up2 = ways()[1]
    put_both((e_out, o_out), up2, 0, [], [u[1:2], u[7:8]], [u[0:1], u[6:7]])


def sweep_kernel(back, med, final, e2, o2, e1, o1, own, got, ginv, out, coords, kept, kept_row, sems):
    def copy(row, source):
        return pltpu.make_async_copy(source, out.at[row], sems.at[row])

    copies = [copy(3, final)]
    copies[0].start()
    coef = jnp.sum(got[...], axis=0)
    kept_row[...] = to_row(jnp.sum(ginv[...] * coef, axis=1, keepdims=True))
    copies.append(pltpu.make_async_copy(kept_row, coords, sems.at[4]))
    copies[1].start()
    ok = flags()
    loads = [back[8:14], back[14:18], back[18:20]]
    b1, a1, b2, a2 = halo_of((e1, o1), (e2, o2))
    u = own[...]
    p = cat(
        only(ok[2], b2[0:1]), only(ok[0], b1[0:2]), u[0:2], only(ok[1], a1[0:2]), only(ok[3], a2[0:1])
    )
    vx = cat(b1[2:4], u[2:4], a1[2:4])
    vy = cat(b1[4:6], u[4:6], a1[4:6])
    vz = cat(b2[1:2], b1[6:8], u[6:8], a1[6:8])
    points = advance_many(p, vx, vy, vz, med[1:7], DT, 3, ok[0], ok[2], loads)
    for i in range(3):
        kept[i] = points[i]
        copies.append(copy(i, kept.at[i]))
        copies[-1].start()
    for each in copies:
        each.wait()


def body(speed, forcing, guess, basis):
    columns = basis.reshape(RANK * 8 * NX, NY)
    state = (8, NX, NY)
    table = [pltpu.VMEM((RANK, NY), F32)]
    split = [pltpu.VMEM((3 * RANK, 16 * NY), BF16)]
    copies = (N_SP, 1, NY)
    far = [(6, NX, NY), (6, NX, NY)]

    def traded(near, distant, center, by_tm):
        far_second = trade(distant[1], by_tm, 2, False)
        far_first = trade(distant[0], by_tm, 2, True)
        near_second = trade(near[1], by_tm, 1, False)
        near_first = trade(near[0], by_tm, 1, True)
        result = [far_first, far_second, near_first, near_second]
        if by_tm:
            result.append(hop(center, by_tm))
        return result

    start = hop(guess.reshape(state), 2)
    load = hop(forcing, 1)
    (c2,) = call(stage_kernel, [(2, NX, NY)], speed, columns)
    e1, o1, e2, o2 = call(
        pack_kernel, [(15, NX, NY), (15, NX, NY), (8, NX, NY), (8, NX, NY)], start, load, c2
    )
    e2, o2, e1, o1 = traded((e1, o1), (e2, o2), None, 0)
    (gram,) = call(
        functools.partial(gram_kernel, (0, 4)), [(RANK, NY)], columns, scratch=split, flops=50_000_000
    )
    relaxed, e, o, med, loads = call(
        relax_kernel,
        [state, *far, (8, NX, NY), (sum(LOADS), NX, NY)],
        start,
        load,
        c2,
        e1,
        o1,
        e2,
        o2,
    )
    near = traded((relaxed, relaxed), (e, o), relaxed, 1)
    (gram,) = call(
        functools.partial(gram_kernel, (4, 8)), [(RANK, NY)], columns, gram, scratch=split, flops=50_000_000
    )
    x, back = call(residue_kernel, [state, (20, NX, NY)], relaxed, loads, med, *near)
    back = hop(back, -1)
    (rows,) = call(first_kernel, [(N_SP, RANK // 2 + 8, NY)], columns, x, gram, scratch=table)
    ginv, *packed = call(
        first_project_kernel, [(RANK, NY), *PROJECTED], share(rows), columns, x, scratch=table
    )

    def exchanged(packed, by_tm):
        center, e1, o1, e2, o2 = packed
        result = traded((e1, o1), (e2, o2), center, by_tm)
        return result if by_tm else result + [center]

    acc = x
    for _ in range(2):
        u, acc, rows = call(
            level_kernel, [state, state, copies], med, *exchanged(packed, 1), acc, columns, scratch=table
        )
        packed = call(project_kernel, PROJECTED, share(rows), ginv, columns, u, scratch=table)
    gap, acc, e, o = call(gap_kernel, [state, state, *far], med, *exchanged(packed, 1), acc)
    e = trade(e, 4, 1, True)
    o = trade(o, 4, 1, False)
    gap = hop(gap, 4)
    x, rows = call(
        chain_kernel, [state, copies], med, o, e, gap, acc, columns, scratch=table
    )
    packed = call(project_kernel, PROJECTED, share(rows), ginv, columns, x, scratch=table)
    final, e, o = call(
        final_kernel,
        [state, (2, NX, NY), (2, NX, NY)],
        med,
        *exchanged(packed, 0),
        back,
    )
    near = traded((final, final), (e, o), final, 1)
    (rows,) = call(products_kernel, [copies], columns, final, scratch=table)
    got = share(rows)
    states, coords = call(
        sweep_kernel,
        [(4, 8, NX, NY), (1, NY)],
        back,
        med,
        final,
        *near,
        got,
        ginv,
        scratch=[pltpu.VMEM((3, 8, NX, NY), F32), pltpu.VMEM((1, NY), F32), pltpu.SemaphoreType.DMA((5,))],
        outward=True,
    )
    return states.reshape(4, 4, 2, NX, NY), coords[:, :RANK]


def solution(mesh):
    placed = (
        P("space", None, None),
        P("tm", "space", None, None),
        P("tm", None, "space", None, None),
        P("tm", None, None, "space", None, None),
    )
    return jax.shard_map(
        body,
        mesh=mesh,
        in_specs=placed,
        out_specs=(P("tm", None, "space", None, None), P("tm", None)),
        check_vma=False,
    )
```
